32 devices in a mesh: section: 4 (over y, core), seq: 8 (over z, x).
Axes of the slice: x: 2, y: 2, z: 4, core: 2. Of those that a mesh axis runs over, the one named last changes fastest.
Arguments:
- stream: bfloat16 [4, 512, 1024], P('section', 'seq'), may hold values from -1.5 to 1.5
- queries: bfloat16 [4, 512, 1024], P('section', 'seq'), may hold values from -8 to 8
- key_rows: bfloat16 [4, 512, 1024], P('section', 'seq'), may hold values from -8 to 8
- values: bfloat16 [4, 512, 1024], P('section', 'seq'), may hold values from -36 to 36
- incoming: bfloat16 [512, 1024], P('seq'), may hold values from -1.5 to 1.5
Outputs:
- updated: bfloat16 [4, 512, 1024], P('section', 'seq')
- received: bfloat16 [4, 512, 1024], P('section', 'seq')
The draws below stay inside these ranges and needn't reach their ends.
All inputs are finite; a program needn't handle non-finite values.
Results may differ from the reference program's by a relative error of at most 0.0054.
Values may be sent and summed in bfloat16 or wider, within the bound.
A program may use at most 64 MiB of HBM per device.

```python
import jax
import jax.numpy as jnp
from jax import lax

HEAD_SIZE = 128
D = 1024
TOKENS = 512
SEQ_LEN = 512
SEQS = 1
SECTIONS = 4


def make_pair(key):
    shape = (SECTIONS, TOKENS, D)
    query_key = jax.random.fold_in(key, 101)
    other_key = jax.random.fold_in(key, 102)
    queries = jnp.clip(jax.random.normal(query_key, shape, jnp.float32), -6.0, 6.0)
    keys_all = jnp.clip(jax.random.normal(other_key, shape, jnp.float32), -6.0, 6.0)
    return (queries, keys_all)


def draw_queries(key, part):
    return make_pair(key)[0].astype(jnp.bfloat16)


def draw_key_rows(key, part):
    return make_pair(key)[1].astype(jnp.bfloat16)


def steps_of(key, extent, shards, smallest, largest):
    gain, own = 1.0, jax.random.fold_in(key, 6)
    for dim, blocks in shards:
        steps = jnp.exp(jax.random.uniform(jax.random.fold_in(own, dim), (blocks,), jnp.float32, smallest / len(shards), largest / len(shards)))
        gain = gain * jnp.repeat(steps, extent[dim] // blocks).reshape([-1 if axis == dim else 1 for axis in range(len(extent))])
    return gain


def gaussian(rng, shape, deviation, limit, cuts=(), held_as=jnp.bfloat16):
    drawn = jax.random.normal(rng, shape, jnp.float32) * deviation
    if len(cuts) > 0:
        drawn = steps_of(rng, shape, cuts, -0.22, 0.18) * drawn
    return jnp.clip(drawn, min=-limit, max=limit).astype(held_as)


def setup_inputs(seed: int = 0) -> dict:
    key_of = jax.random.split(jax.random.key(seed), 6)
    return {
        "stream": gaussian(key_of[0], (SECTIONS, TOKENS, D), 0.25, 1.5, ((0, 4), (1, 8))),
        "queries": draw_queries(jax.random.fold_in(key_of[5], 71), 0),
        "key_rows": draw_key_rows(jax.random.fold_in(key_of[5], 71), 0),
        "values": gaussian(key_of[3], (SECTIONS, TOKENS, D), 6.0, 36.0, ((0, 4), (1, 8))),
        "incoming": gaussian(key_of[4], (TOKENS, D), 0.25, 1.5, ((0, 8),)),
    }


def attend_sequence(pieces):
    query_rows, key_rows, value_rows = pieces
    tok_count = query_rows.shape[0]
    head_count = query_rows.shape[1] // HEAD_SIZE
    query_f = query_rows.astype(jnp.float32).reshape(tok_count, head_count, HEAD_SIZE)
    key_f = key_rows.astype(jnp.float32).reshape(tok_count, head_count, HEAD_SIZE)
    value_f = value_rows.astype(jnp.float32).reshape(tok_count, head_count, HEAD_SIZE)
    scale = HEAD_SIZE ** -0.5
    scores = jnp.einsum("qhd,khd->hqk", query_f, key_f) * scale
    highest = jnp.max(scores, axis=-1, keepdims=True)
    exponent = jnp.exp(scores - highest)
    totals = jnp.sum(exponent, axis=-1)
    weights = lax.optimization_barrier(exponent.astype(jnp.bfloat16)).astype(jnp.float32)
    summed = jnp.einsum("hqk,khd->qhd", weights, value_f)
    attended = (summed / jnp.transpose(totals)[:, :, None]).astype(jnp.bfloat16)
    return attended.reshape(tok_count, head_count * HEAD_SIZE)


def attend_section(pieces):
    query_rows, key_rows, value_rows, stream_rows = pieces
    width = query_rows.shape[1]
    query_seq = query_rows.reshape(SEQS, SEQ_LEN, width)
    key_seq = key_rows.reshape(SEQS, SEQ_LEN, width)
    value_seq = value_rows.reshape(SEQS, SEQ_LEN, width)
    attended = lax.map(attend_sequence, (query_seq, key_seq, value_seq)).reshape(TOKENS, width)
    return (stream_rows.astype(jnp.float32) + attended.astype(jnp.float32)).astype(jnp.bfloat16)


def reference(stream, queries, key_rows, values, incoming):
    updated = lax.map(attend_section, (queries, key_rows, values, stream))
    received = jnp.concatenate([incoming[None], updated[:-1]], axis=0)
    return updated, received
```

```python
import functools

import jax
import jax.numpy as jnp
from jax import lax
from jax.experimental import pallas as pl
from jax.experimental.pallas import tpu as pltpu
from jax.sharding import PartitionSpec as P

HEAD_SIZE = 128
GROUP = 8
LOG2_E = 1.4426950408889634
MESH = pl.DeviceIdType.MESH
KEY_VALUE = (0, 1)
QUERY = (2,)
ALL = (0, 1, 2)
QUERY_FIRST = (2, 0, 1)
SEND_ORDER = (
    ((4, KEY_VALUE), (1, KEY_VALUE), (5, KEY_VALUE), (6, KEY_VALUE), (7, KEY_VALUE), (3, KEY_VALUE), (2, KEY_VALUE), (1, QUERY), (6, QUERY), (7, QUERY), (4, QUERY), (5, QUERY), (3, QUERY), (2, QUERY)),
    ((4, KEY_VALUE), (1, KEY_VALUE), (5, KEY_VALUE), (6, KEY_VALUE), (7, KEY_VALUE), (3, KEY_VALUE), (2, KEY_VALUE), (1, QUERY), (6, QUERY), (7, QUERY), (4, QUERY), (5, QUERY), (3, QUERY), (2, QUERY)),
    ((4, KEY_VALUE), (1, KEY_VALUE), (5, KEY_VALUE), (6, KEY_VALUE), (7, KEY_VALUE), (3, KEY_VALUE), (2, KEY_VALUE), (1, QUERY), (6, QUERY), (7, QUERY), (4, QUERY), (5, QUERY), (3, QUERY), (2, QUERY)),
    ((4, KEY_VALUE), (1, KEY_VALUE), (5, KEY_VALUE), (6, KEY_VALUE), (7, KEY_VALUE), (3, KEY_VALUE), (2, KEY_VALUE), (1, QUERY), (6, QUERY), (7, QUERY), (4, QUERY), (5, QUERY), (3, QUERY), (2, QUERY)),
    ((4, KEY_VALUE), (1, KEY_VALUE), (5, KEY_VALUE), (6, KEY_VALUE), (7, KEY_VALUE), (3, KEY_VALUE), (2, KEY_VALUE), (1, QUERY), (6, QUERY), (7, QUERY), (4, QUERY), (5, QUERY), (3, QUERY), (2, QUERY)),
    ((4, KEY_VALUE), (1, KEY_VALUE), (5, KEY_VALUE), (6, KEY_VALUE), (7, KEY_VALUE), (3, KEY_VALUE), (2, KEY_VALUE), (1, QUERY), (6, QUERY), (7, QUERY), (4, QUERY), (5, QUERY), (3, QUERY), (2, QUERY)),
    ((4, KEY_VALUE), (1, KEY_VALUE), (5, KEY_VALUE), (6, KEY_VALUE), (7, KEY_VALUE), (3, KEY_VALUE), (2, KEY_VALUE), (1, QUERY), (6, QUERY), (7, QUERY), (4, QUERY), (5, QUERY), (3, QUERY), (2, QUERY)),
    ((4, KEY_VALUE), (1, KEY_VALUE), (5, KEY_VALUE), (6, KEY_VALUE), (7, KEY_VALUE), (3, KEY_VALUE), (2, KEY_VALUE), (1, QUERY), (6, QUERY), (7, QUERY), (4, QUERY), (5, QUERY), (3, QUERY), (2, QUERY)),
    ((4, KEY_VALUE), (1, KEY_VALUE), (5, KEY_VALUE), (6, KEY_VALUE), (7, KEY_VALUE), (3, KEY_VALUE), (2, KEY_VALUE), (1, QUERY), (6, QUERY), (7, QUERY), (4, QUERY), (5, QUERY), (3, QUERY), (2, QUERY)),
    ((4, KEY_VALUE), (1, KEY_VALUE), (5, KEY_VALUE), (6, KEY_VALUE), (7, KEY_VALUE), (3, KEY_VALUE), (2, KEY_VALUE), (1, QUERY), (6, QUERY), (7, QUERY), (4, QUERY), (5, QUERY), (3, QUERY), (2, QUERY)),
    ((4, KEY_VALUE), (1, KEY_VALUE), (5, KEY_VALUE), (6, KEY_VALUE), (7, KEY_VALUE), (3, KEY_VALUE), (2, KEY_VALUE), (1, QUERY), (6, QUERY), (7, QUERY), (4, QUERY), (5, QUERY), (3, QUERY), (2, QUERY)),
    ((4, KEY_VALUE), (1, KEY_VALUE), (5, KEY_VALUE), (6, KEY_VALUE), (7, KEY_VALUE), (3, KEY_VALUE), (2, KEY_VALUE), (1, QUERY), (6, QUERY), (7, QUERY), (4, QUERY), (5, QUERY), (3, QUERY), (2, QUERY)),
    ((4, KEY_VALUE), (1, KEY_VALUE), (5, KEY_VALUE), (6, KEY_VALUE), (7, KEY_VALUE), (3, KEY_VALUE), (2, KEY_VALUE), (1, QUERY), (6, QUERY), (7, QUERY), (4, QUERY), (5, QUERY), (3, QUERY), (2, QUERY)),
    ((4, KEY_VALUE), (1, KEY_VALUE), (5, KEY_VALUE), (6, KEY_VALUE), (7, KEY_VALUE), (3, KEY_VALUE), (2, KEY_VALUE), (1, QUERY), (6, QUERY), (7, QUERY), (4, QUERY), (5, QUERY), (3, QUERY), (2, QUERY)),
    ((4, KEY_VALUE), (1, KEY_VALUE), (5, KEY_VALUE), (6, KEY_VALUE), (7, KEY_VALUE), (3, KEY_VALUE), (2, KEY_VALUE), (1, QUERY), (6, QUERY), (7, QUERY), (4, QUERY), (5, QUERY), (3, QUERY), (2, QUERY)),
    ((4, KEY_VALUE), (1, KEY_VALUE), (5, KEY_VALUE), (6, KEY_VALUE), (7, KEY_VALUE), (3, KEY_VALUE), (2, KEY_VALUE), (1, QUERY), (6, QUERY), (7, QUERY), (4, QUERY), (5, QUERY), (3, QUERY), (2, QUERY)),
)
SERVE_ORDER = (((3, 1), (2, 1), (1, 1), (0, 1)), ((2, 1), (0, 1), (1, 1), (3, 1)), ((2, 1), (0, 1), (1, 1), (3, 1)), ((3, 1), (2, 1), (1, 1), (0, 1)))
UPDATE_ORDER = ((0, 1, 2, 3),) * 4


def flipped(place, mask):
    result, weight = 0, 1
    while weight < GROUP:
        bit = lax.rem(lax.div(place, weight), 2)
        result = result + weight * ((1 - bit) if mask & weight else bit)
        weight *= 2
    return result


def kernel(
    sections,
    stream_hbm, query_hbm, key_hbm, value_hbm, incoming_hbm,
    both_ref,
    stream_own, held, key_all, value_all, query_all, result, attended,
    load_sem, send_sem, recv_sem, query_sem, back_sem, known_sem,
):
    updated_ref, received_ref = both_ref.at[0], both_ref.at[1]
    section = lax.axis_index("section")
    seq = lax.axis_index("seq")
    me = lax.rem(seq, GROUP)
    base = seq - me
    row = lax.div(me, 2)
    width = query_all.shape[2]
    place = {mask: flipped(me, mask) for mask in range(GROUP)}
    others = pl.ds(1, GROUP - 1)

    def columns(mask):
        return pl.ds(pl.multiple_of(place[mask] * width, HEAD_SIZE), width)

    whole = (key_all, value_all, query_all)
    loads = [
        pltpu.make_async_copy(source, held.at[kind], load_sem.at[0])
        for kind, source in enumerate((key_hbm, value_hbm, query_hbm))
    ]
    for load in loads:
        load.start()

    side = lax.rem(me, 2)
    barrier = pltpu.get_barrier_semaphore()
    for mask in range(1, GROUP):
        later_row = place[mask] > me + 1 - side
        if mask == 1:
            greets = (side == 0) | (row == 0)
        elif mask % 2:
            greets = later_row & (side == 0)
        else:
            greets = later_row

        @pl.when(greets)
        def _():
            pl.semaphore_signal(
                barrier, inc=1, device_id={"seq": base + place[mask]}, device_id_type=MESH
            )

    @pl.when(section < sections - 1)
    def _():
        pl.semaphore_signal(barrier, inc=1, device_id={"section": section + 1}, device_id_type=MESH)

    stream_load = pltpu.make_async_copy(stream_hbm, stream_own, load_sem.at[1])
    stream_load.start()
    first = pltpu.make_async_copy(incoming_hbm, received_ref, load_sem.at[2])

    @pl.when(section == 0)
    def _():
        first.start()

    def exchange(kind, mask):
        return pltpu.make_async_remote_copy(
            src_ref=held.at[kind, :, columns(mask)],
            dst_ref=whole[kind].at[mask],
            send_sem=send_sem.at[kind],
            recv_sem=query_sem.at[mask // 2] if kind == 2 else recv_sem.at[kind],
            device_id={"seq": base + place[mask]},
            device_id_type=MESH,
        )

    def giving_back(mask):
        return pltpu.make_async_remote_copy(
            src_ref=result.at[mask],
            dst_ref=attended.at[mask],
            send_sem=send_sem.at[3],
            recv_sem=back_sem.at[mask // 2],
            device_id={"seq": base + place[mask]},
            device_id_type=MESH,
        )

    def passing(cols):
        return pltpu.make_async_remote_copy(
            src_ref=updated_ref.at[:, cols],
            dst_ref=received_ref.at[:, cols],
            send_sem=send_sem.at[4],
            recv_sem=recv_sem.at[2],
            device_id={"section": lax.rem(section + 1, sections)},
            device_id_type=MESH,
        )

    def landed(ref, sem):
        pltpu.make_async_copy(ref, ref, sem).wait()

    greeted = jnp.where(side == 0, jnp.maximum(row, 1), 2 * row + 1)
    pl.semaphore_wait(barrier, greeted + jnp.where(section > 0, 1, 0))
    for mask in (6, 4, 2, 7, 5, 3, 1):
        earlier_row = place[mask] < me - side
        if mask == 1:
            answers = (side == 1) & (row > 0)
        elif mask % 2:
            answers = earlier_row & (side == 1)
        else:
            answers = earlier_row

        @pl.when(answers)
        def _():
            pl.semaphore_signal(
                known_sem.at[mask], inc=1,
                device_id={"seq": base + place[mask]}, device_id_type=MESH,
            )

    @pl.when(section > 0)
    def _():
        pl.semaphore_signal(
            known_sem.at[0], inc=1, device_id={"section": section - 1}, device_id_type=MESH
        )

    def by_place(orders, run):
        for number, order in enumerate(orders):
            if order:

                @pl.when(me + GROUP * lax.rem(section, 2) == number)
                def _():
                    run(number % GROUP, order)

    def notices(mine, mask):
        theirs = mine ^ mask
        if theirs // 2 > mine // 2:
            return mask - mask % 2 * (mine % 2)
        if mine % 2 == 0 and theirs % 2 and mine > 0:
            return 1
        return 0

    def send(mine, order):
        met = {0}
        for mask, kinds in order:
            notice = notices(mine, mask)
            if notice not in met:
                met.add(notice)
                pl.semaphore_wait(known_sem.at[notice], 1)
            for kind in kinds:
                exchange(kind, mask).start()

    def by_row(orders, run):
        for order in sorted(set(orders)):
            rows = [number for number, its in enumerate(orders) if its == order]
            here = row == rows[0]
            for number in rows[1:]:
                here = here | (row == number)

            @pl.when(here)
            def _():
                run(order)

    landed(held, load_sem.at[0])
    by_place(SEND_ORDER, send)
    for kind in range(3):
        whole[kind][0] = held[kind, :, columns(0)]
    landed(stream_own, load_sem.at[1])
    landed(key_all.at[others], recv_sem.at[0])
    landed(value_all.at[others], recv_sem.at[1])

    factor = HEAD_SIZE ** -0.5 * LOG2_E

    def attend(pair, count):
        at = pl.ds(2 * pair, 2 * count)
        for start in range(0, width, HEAD_SIZE):
            feats = pl.ds(start, HEAD_SIZE)
            keys = key_all[:, :, feats].reshape(-1, HEAD_SIZE)
            vals = value_all[:, :, feats].reshape(-1, HEAD_SIZE)
            scores = lax.dot_general(
                query_all[at, :, feats].reshape(-1, HEAD_SIZE), keys, (((1,), (1,)), ((), ())),
                preferred_element_type=jnp.float32,
            )
            highest = jnp.max(scores, axis=-1, keepdims=True)
            exponent = jnp.exp2((scores - highest) * factor)
            totals = jnp.sum(exponent, axis=-1, keepdims=True)
            summed = jnp.dot(
                exponent.astype(jnp.bfloat16), vals, preferred_element_type=jnp.float32
            )
            out = (summed * (1.0 / totals)).astype(jnp.bfloat16)
            result[at, :, feats] = out.reshape(2 * count, -1, HEAD_SIZE)

    def pieces(pair):
        return pl.ds(2 * pair, 2) if pair else pl.ds(1, 1)

    def serve(order):
        for pair, count in order:
            for number in range(pair, pair + count):
                landed(query_all.at[pieces(number)], query_sem.at[number])
            attend(pair, count)
            for mask in range(2 * pair, 2 * (pair + count)):
                if mask:
                    giving_back(mask).start()

    by_row(SERVE_ORDER, serve)

    def update(mask, piece):
        cols = columns(mask)
        updated_ref[:, cols] = (
            stream_own[:, cols].astype(jnp.float32) + piece.astype(jnp.float32)
        ).astype(jnp.bfloat16)

    def finish(order):
        for pair in order:
            landed(attended.at[pieces(pair)], back_sem.at[pair])
            update(2 * pair, attended[2 * pair] if pair else result[0])
            update(2 * pair + 1, attended[2 * pair + 1])

            @pl.when(section < sections - 1)
            def _():
                low = jnp.minimum(place[2 * pair], place[2 * pair + 1])
                passing(pl.ds(pl.multiple_of(low * width, HEAD_SIZE), 2 * width)).start()

    @pl.when(section < sections - 1)
    def _():
        pl.semaphore_wait(known_sem.at[0], 1)

    by_row(UPDATE_ORDER, finish)

    for kind in range(4):
        landed(key_all.at[others], send_sem.at[kind])

    @pl.when(section < sections - 1)
    def _():
        landed(updated_ref, send_sem.at[4])

    @pl.when(section > 0)
    def _():
        landed(received_ref, recv_sem.at[2])

    @pl.when(section == 0)
    def _():
        first.wait()


def per_device(sections, stream, queries, key_rows, values, incoming):
    rows, features = incoming.shape
    width = features // GROUP
    whole = pltpu.VMEM((GROUP, rows, width), jnp.bfloat16)
    both = pl.pallas_call(
        functools.partial(kernel, sections),
        out_shape=pltpu.VMEM((2, rows, features), jnp.bfloat16),
        in_specs=[pl.BlockSpec(memory_space=pl.ANY)] * 5,
        out_specs=pl.BlockSpec(memory_space=pltpu.VMEM),
        scratch_shapes=[
            pltpu.VMEM((rows, features), jnp.bfloat16),
            pltpu.VMEM((3, rows, features), jnp.bfloat16),
        ] + [whole] * 5 + [
            pltpu.SemaphoreType.DMA((3,)),
            pltpu.SemaphoreType.DMA((5,)),
            pltpu.SemaphoreType.DMA((3,)),
            pltpu.SemaphoreType.DMA((GROUP // 2,)),
            pltpu.SemaphoreType.DMA((GROUP // 2,)),
            pltpu.SemaphoreType.REGULAR((GROUP,)),
        ],
        compiler_params=pltpu.CompilerParams(collective_id=0, has_side_effects=True),
    )(stream[0], queries[0], key_rows[0], values[0], incoming)
    return both[:1], both[1:]


def solution(mesh):
    placed = (
        P("section", "seq", None),
        P("section", "seq", None),
        P("section", "seq", None),
        P("section", "seq", None),
        P("seq", None),
    )
    return jax.shard_map(
        functools.partial(per_device, mesh.shape["section"]),
        mesh=mesh,
        in_specs=placed,
        out_specs=(P("section", "seq", None), P("section", "seq", None)),
        check_vma=False,
    )
```

```python
import functools

import jax
import jax.numpy as jnp
from jax import lax
from jax.experimental import pallas as pl
from jax.experimental.pallas import tpu as pltpu
from jax.sharding import PartitionSpec as P

HEAD_SIZE = 128
GROUP = 8
WORKERS = (2, 3, 4, 5)
LOG2_E = 1.4426950408889634
MESH = pl.DeviceIdType.MESH
KEY_VALUE, QUERY, ALL = (0, 1), (2,), (0, 1, 2)
SEND_ORDER = (
    ((2, QUERY), (3, KEY_VALUE), (3, QUERY), (4, QUERY), (5, QUERY), (4, KEY_VALUE), (5, KEY_VALUE), (2, KEY_VALUE)),
    ((3, QUERY), (2, KEY_VALUE), (2, QUERY), (5, QUERY), (4, QUERY), (5, KEY_VALUE), (4, KEY_VALUE), (3, KEY_VALUE)),
    ((4, KEY_VALUE), (5, KEY_VALUE), (3, KEY_VALUE), (4, QUERY), (5, QUERY), (3, QUERY)),
    ((5, KEY_VALUE), (4, KEY_VALUE), (2, KEY_VALUE), (5, QUERY), (4, QUERY), (2, QUERY)),
    ((2, KEY_VALUE), (3, KEY_VALUE), (5, KEY_VALUE), (2, QUERY), (3, QUERY), (5, QUERY)),
    ((3, KEY_VALUE), (2, KEY_VALUE), (4, KEY_VALUE), (3, QUERY), (2, QUERY), (4, QUERY)),
    ((2, KEY_VALUE), (3, KEY_VALUE), (4, KEY_VALUE), (5, KEY_VALUE), (2, QUERY), (3, QUERY), (4, QUERY), (5, QUERY)),
    ((3, KEY_VALUE), (2, KEY_VALUE), (5, KEY_VALUE), (4, KEY_VALUE), (3, QUERY), (2, QUERY), (5, QUERY), (4, QUERY)),
    ((None, 500), (2, KEY_VALUE), (3, KEY_VALUE), (4, KEY_VALUE), (5, KEY_VALUE), (None, 1000), (4, QUERY), (5, QUERY), (2, QUERY), (3, QUERY)),
    ((None, 500), (3, KEY_VALUE), (2, KEY_VALUE), (5, KEY_VALUE), (4, KEY_VALUE), (None, 1000), (5, QUERY), (4, QUERY), (3, QUERY), (2, QUERY)),
    ((None, 500), (4, KEY_VALUE), (5, KEY_VALUE), (3, KEY_VALUE), (None, 1000), (4, QUERY), (5, QUERY), (3, QUERY)),
    ((None, 500), (5, KEY_VALUE), (4, KEY_VALUE), (2, KEY_VALUE), (None, 1000), (5, QUERY), (4, QUERY), (2, QUERY)),
    ((None, 500), (2, KEY_VALUE), (3, KEY_VALUE), (5, KEY_VALUE), (None, 1000), (2, QUERY), (3, QUERY), (5, QUERY)),
    ((None, 500), (3, KEY_VALUE), (2, KEY_VALUE), (4, KEY_VALUE), (None, 1000), (3, QUERY), (2, QUERY), (4, QUERY)),
    ((None, 500), (2, KEY_VALUE), (3, KEY_VALUE), (4, KEY_VALUE), (5, KEY_VALUE), (None, 1000), (2, QUERY), (3, QUERY), (4, QUERY), (5, QUERY)),
    ((None, 500), (3, KEY_VALUE), (2, KEY_VALUE), (5, KEY_VALUE), (4, KEY_VALUE), (None, 1000), (3, QUERY), (2, QUERY), (5, QUERY), (4, QUERY)),
)
LATE_ORDER = (
    (),
    (),
    (),
    (),
    (),
    (),
    (),
    (),
    (),
    (),
    (),
    (),
    (),
    (),
    (),
    (),
)
SERVE_ORDER = (((1, 1), (3, 1), (2, 1), (0, 1)), ((2, 1), (3, 1), (0, 1), (1, 1)))
FINISH_ORDER = ((2, 3, 4, 5), (2, 3, 4, 5), (2, 3, 4, 5), (2, 3, 4, 5))


def notice(mine, theirs):
    if theirs // 2 > mine // 2:
        return theirs if mine % 2 == 0 else theirs | 1
    if mine % 2 == 0 and theirs % 2 and mine > 0:
        return mine + 1
    return None


def notices(mine):
    return {notice(mine, theirs) for theirs in WORKERS if theirs != mine} - {None}


def kernel(
    sections,
    stream_hbm, query_hbm, key_hbm, value_hbm, incoming_hbm,
    both_ref,
    stream_own, held, gathered, result, attended,
    load_sem, send_sem, recv_sem, query_sem, back_sem, known_sem,
):
    updated_ref, received_ref = both_ref.at[0], both_ref.at[1]
    key_all, value_all, query_all = (gathered.at[kind] for kind in range(3))
    section = lax.axis_index("section")
    seq = lax.axis_index("seq")
    me = lax.rem(seq, GROUP)
    base = seq - me
    row, side = lax.div(me, 2), lax.rem(me, 2)
    width = gathered.shape[3]
    others = pl.ds(1, GROUP - 1)
    working = (me >= WORKERS[0]) & (me <= WORKERS[-1])

    loads = [
        pltpu.make_async_copy(source, held.at[kind], load_sem.at[0])
        for kind, source in enumerate((key_hbm, value_hbm, query_hbm))
    ]
    for load in loads:
        load.start()

    def here(run):
        for mine in range(GROUP):

            @pl.when(me == mine)
            def _():
                run(mine)

    def signal(sem, place):
        pl.semaphore_signal(sem, inc=1, device_id={"seq": base + place}, device_id_type=MESH)

    barrier = pltpu.get_barrier_semaphore()

    def greet(mine):
        for theirs in range(GROUP):
            later = theirs // 2 > mine // 2 and (mine % 2 == 0 or theirs % 2)
            if later or theirs == mine + 1 - mine % 2 * 2 and (mine % 2 == 0 or mine == 1):
                signal(barrier, theirs)

    here(greet)

    @pl.when(section < sections - 1)
    def _():
        pl.semaphore_signal(barrier, inc=1, device_id={"section": section + 1}, device_id_type=MESH)

    stream_load = pltpu.make_async_copy(stream_hbm, stream_own, load_sem.at[1])
    stream_load.start()

    @pl.when(section == 0)
    def _():
        pltpu.make_async_copy(incoming_hbm, received_ref, recv_sem.at[1]).start()

    def exchange(kind, mine, theirs):
        return pltpu.make_async_remote_copy(
            src_ref=held.at[kind, :, pl.ds((theirs - WORKERS[0]) * width, width)],
            dst_ref=gathered.at[kind, mine ^ theirs],
            send_sem=send_sem.at[3 if kind == 2 else 0],
            recv_sem=query_sem.at[(mine ^ theirs) // 2] if kind == 2 else recv_sem.at[0],
            device_id={"seq": base + theirs},
            device_id_type=MESH,
        )

    def giving_back(mask):
        place = 0
        for weight in (1, 2, 4):
            bit = lax.rem(lax.div(me, weight), 2)
            place = place + weight * ((1 - bit) if mask & weight else bit)
        return pltpu.make_async_remote_copy(
            src_ref=result.at[mask],
            dst_ref=attended.at[me - WORKERS[0]],
            send_sem=send_sem.at[1],
            recv_sem=back_sem.at[me - WORKERS[0]],
            device_id={"seq": base + place},
            device_id_type=MESH,
        )

    def passing(cols):
        return pltpu.make_async_remote_copy(
            src_ref=updated_ref.at[:, cols],
            dst_ref=received_ref.at[:, cols],
            send_sem=send_sem.at[2],
            recv_sem=recv_sem.at[1],
            device_id={"section": lax.rem(section + 1, sections)},
            device_id_type=MESH,
        )

    def landed(ref, sem):
        pltpu.make_async_copy(ref, ref, sem).wait()

    greeted = jnp.where(side == 0, jnp.maximum(row, 1), 2 * row + 1)
    pl.semaphore_wait(barrier, greeted + jnp.where(section > 0, 1, 0))

    def answer(mine):
        for theirs in range(GROUP):
            if mine in notices(theirs):
                signal(known_sem.at[mine ^ theirs], theirs)

    here(answer)

    @pl.when(section > 0)
    def _():
        pl.semaphore_signal(
            known_sem.at[0], inc=1, device_id={"section": section - 1}, device_id_type=MESH
        )

    landed(held, load_sem.at[0])
    def send(orders, earlier):
        for number, order in enumerate(orders):
            mine, met = number % GROUP, {None}
            for theirs, _ in earlier[number]:
                if theirs is not None:
                    met.add(notice(mine, theirs))
            if order:

                @pl.when(me + GROUP * lax.rem(section, 2) == number)
                def _():
                    for theirs, kinds in order:
                        if theirs is None:
                            pl.delay(kinds)
                            continue
                        shown = notice(mine, theirs)
                        if shown not in met:
                            met.add(shown)
                            pl.semaphore_wait(known_sem.at[mine ^ shown], 1)
                        for kind in kinds:
                            exchange(kind, mine, theirs).start()

    send(SEND_ORDER, [()] * len(SEND_ORDER))

    factor = HEAD_SIZE ** -0.5 * LOG2_E

    def attend(pair, count):
        at = pl.ds(2 * pair, 2 * count)
        for start in range(0, width, 2 * HEAD_SIZE):
            heads = [pl.ds(start + offset, HEAD_SIZE) for offset in (0, HEAD_SIZE)]
            scores = [
                lax.dot_general(
                    query_all[at, :, head].reshape(-1, HEAD_SIZE),
                    key_all[:, :, head].reshape(-1, HEAD_SIZE),
                    (((1,), (1,)), ((), ())),
                    preferred_element_type=jnp.float32,
                )
                for head in heads
            ]
            highest = [jnp.max(its, axis=-1, keepdims=True) for its in scores]
            exponent = [jnp.exp2((its - top) * factor) for its, top in zip(scores, highest)]
            totals = [jnp.sum(its, axis=-1, keepdims=True) for its in exponent]
            summed = [
                jnp.dot(
                    its.astype(jnp.bfloat16), value_all[:, :, head].reshape(-1, HEAD_SIZE),
                    preferred_element_type=jnp.float32,
                )
                for its, head in zip(exponent, heads)
            ]
            for its, total, head in zip(summed, totals, heads):
                out = (its * (1.0 / total)).astype(jnp.bfloat16)
                result[at, :, head] = out.reshape(2 * count, -1, HEAD_SIZE)

    @pl.when(working)
    def _():
        own = pl.ds(pl.multiple_of((me - WORKERS[0]) * width, HEAD_SIZE), width)
        for kind in range(3):
            gathered[kind, 0] = held[kind, :, own]
        landed(gathered.at[pl.ds(0, 2), others], recv_sem.at[0])

    @pl.when(jnp.logical_not(working))
    def _():
        landed(held.at[pl.ds(0, 2)], send_sem.at[0])

    send(LATE_ORDER, SEND_ORDER)

    for number, order in enumerate(SERVE_ORDER):

        @pl.when(row == WORKERS[0] // 2 + number)
        def _():
            for pair, count in order:
                for its in range(pair, pair + count):
                    landed(query_all.at[pl.ds(2 * its, 2) if its else pl.ds(1, 1)], query_sem.at[its])
                attend(pair, count)
                for mask in range(2 * pair, 2 * (pair + count)):
                    if mask:
                        giving_back(mask).start()

    landed(stream_own, load_sem.at[1])

    @pl.when(section < sections - 1)
    def _():
        pl.semaphore_wait(known_sem.at[0], 1)

    def finish(worker):
        cols = pl.ds((worker - WORKERS[0]) * width, width)

        def update(piece):
            updated_ref[:, cols] = (
                stream_own[:, cols].astype(jnp.float32) + piece.astype(jnp.float32)
            ).astype(jnp.bfloat16)

        @pl.when(me == worker)
        def _():
            update(result[0])

        @pl.when(me != worker)
        def _():
            landed(attended.at[worker - WORKERS[0]], back_sem.at[worker - WORKERS[0]])
            update(attended[worker - WORKERS[0]])

        @pl.when(section < sections - 1)
        def _():
            passing(cols).start()

    for order in sorted(set(FINISH_ORDER)):
        chosen = functools.reduce(
            jnp.logical_or, [row == number for number, its in enumerate(FINISH_ORDER) if its == order]
        )

        @pl.when(chosen)
        def _():
            for worker in order:
                finish(worker)

    @pl.when(working)
    def _():
        most = pl.ds(0, (len(WORKERS) - 1) * width)
        landed(held.at[pl.ds(0, 2), :, most], send_sem.at[0])
        landed(held.at[2, :, most], send_sem.at[3])
        landed(result.at[others], send_sem.at[1])

    @pl.when(jnp.logical_not(working))
    def _():
        landed(held.at[2], send_sem.at[3])

    @pl.when(section < sections - 1)
    def _():
        landed(updated_ref, send_sem.at[2])

    landed(received_ref, recv_sem.at[1])


def per_device(sections, stream, queries, key_rows, values, incoming):
    rows, features = incoming.shape
    width = features // len(WORKERS)
    both = pl.pallas_call(
        functools.partial(kernel, sections),
        out_shape=pltpu.VMEM((2, rows, features), jnp.bfloat16),
        in_specs=[pl.BlockSpec(memory_space=pl.ANY)] * 5,
        out_specs=pl.BlockSpec(memory_space=pltpu.VMEM),
        scratch_shapes=[
            pltpu.VMEM((rows, features), jnp.bfloat16),
            pltpu.VMEM((3, rows, features), jnp.bfloat16),
            pltpu.VMEM((3, GROUP, rows, width), jnp.bfloat16),
            pltpu.VMEM((GROUP, rows, width), jnp.bfloat16),
            pltpu.VMEM((len(WORKERS), rows, width), jnp.bfloat16),
            pltpu.SemaphoreType.DMA((2,)),
            pltpu.SemaphoreType.DMA((4,)),
            pltpu.SemaphoreType.DMA((2,)),
            pltpu.SemaphoreType.DMA((GROUP // 2,)),
            pltpu.SemaphoreType.DMA((len(WORKERS),)),
            pltpu.SemaphoreType.REGULAR((GROUP,)),
        ],
        compiler_params=pltpu.CompilerParams(collective_id=0, has_side_effects=True),
    )(stream[0], queries[0], key_rows[0], values[0], incoming)
    return both[:1], both[1:]


def solution(mesh):
    placed = (
        P("section", "seq", None),
        P("section", "seq", None),
        P("section", "seq", None),
        P("section", "seq", None),
        P("seq", None),
    )
    return jax.shard_map(
        functools.partial(per_device, mesh.shape["section"]),
        mesh=mesh,
        in_specs=placed,
        out_specs=(P("section", "seq", None), P("section", "seq", None)),
        check_vma=False,
    )
```

```python
import functools

import jax
import jax.numpy as jnp
from jax import lax
from jax.experimental import pallas as pl
from jax.experimental.pallas import tpu as pltpu
from jax.sharding import PartitionSpec as P

HEAD_SIZE = 128
GROUP = 8
WORKERS = (2, 3, 4, 5)
LOG2_E = 1.4426950408889634
MESH = pl.DeviceIdType.MESH
KEY_VALUE, QUERY, ALL = (0, 1), (2,), (0, 1, 2)
SEND_ORDER = (
    ((2, QUERY), (3, KEY_VALUE), (3, QUERY), (4, QUERY), (5, QUERY), (4, KEY_VALUE), (5, KEY_VALUE), (2, KEY_VALUE)),
    ((3, QUERY), (2, KEY_VALUE), (2, QUERY), (5, QUERY), (4, QUERY), (5, KEY_VALUE), (4, KEY_VALUE), (3, KEY_VALUE)),
    ((4, KEY_VALUE), (5, KEY_VALUE), (3, KEY_VALUE), (4, QUERY), (5, QUERY), (3, QUERY)),
    ((5, KEY_VALUE), (4, KEY_VALUE), (2, KEY_VALUE), (5, QUERY), (4, QUERY), (2, QUERY)),
    ((2, KEY_VALUE), (3, KEY_VALUE), (5, KEY_VALUE), (2, QUERY), (3, QUERY), (5, QUERY)),
    ((3, KEY_VALUE), (2, KEY_VALUE), (4, KEY_VALUE), (3, QUERY), (2, QUERY), (4, QUERY)),
    ((2, KEY_VALUE), (3, KEY_VALUE), (4, KEY_VALUE), (5, KEY_VALUE), (2, QUERY), (3, QUERY), (4, QUERY), (5, QUERY)),
    ((3, KEY_VALUE), (2, KEY_VALUE), (5, KEY_VALUE), (4, KEY_VALUE), (3, QUERY), (2, QUERY), (5, QUERY), (4, QUERY)),
    ((None, 500), (2, KEY_VALUE), (3, KEY_VALUE), (4, KEY_VALUE), (5, KEY_VALUE), (4, QUERY), (5, QUERY), (2, QUERY), (3, QUERY)),
    ((None, 500), (3, KEY_VALUE), (2, KEY_VALUE), (5, KEY_VALUE), (4, KEY_VALUE), (5, QUERY), (4, QUERY), (3, QUERY), (2, QUERY)),
    ((None, 500), (4, KEY_VALUE), (5, KEY_VALUE), (3, KEY_VALUE), (4, QUERY), (5, QUERY), (3, QUERY)),
    ((None, 500), (5, KEY_VALUE), (4, KEY_VALUE), (2, KEY_VALUE), (5, QUERY), (4, QUERY), (2, QUERY)),
    ((None, 500), (2, KEY_VALUE), (3, KEY_VALUE), (5, KEY_VALUE), (2, QUERY), (3, QUERY), (5, QUERY)),
    ((None, 500), (3, KEY_VALUE), (2, KEY_VALUE), (4, KEY_VALUE), (3, QUERY), (2, QUERY), (4, QUERY)),
    ((None, 500), (2, KEY_VALUE), (3, KEY_VALUE), (4, KEY_VALUE), (5, KEY_VALUE), (2, QUERY), (3, QUERY), (4, QUERY), (5, QUERY)),
    ((None, 500), (3, KEY_VALUE), (2, KEY_VALUE), (5, KEY_VALUE), (4, KEY_VALUE), (3, QUERY), (2, QUERY), (5, QUERY), (4, QUERY)),
)
LATE_ORDER = (
    (),
    (),
    (),
    (),
    (),
    (),
    (),
    (),
    (),
    (),
    (),
    (),
    (),
    (),
    (),
    (),
)
SERVE_ORDER = (((1, 1), (3, 1), (2, 1), (0, 1)), ((2, 1), (3, 1), (0, 1), (1, 1)))
FINISH_ORDER = ((2, 3, 4, 5), (2, 3, 4, 5), (2, 3, 4, 5), (2, 3, 4, 5))


def notice(mine, theirs):
    if theirs // 2 > mine // 2:
        return theirs if mine % 2 == 0 else theirs | 1
    if mine % 2 == 0 and theirs % 2 and mine > 0:
        return mine + 1
    return None


def notices(mine):
    return {notice(mine, theirs) for theirs in WORKERS if theirs != mine} - {None}


def kernel(
    sections,
    stream_hbm, query_hbm, key_hbm, value_hbm, incoming_hbm,
    both_ref,
    stream_own, held, gathered, result, attended, stream_before, attended_before,
    load_sem, send_sem, recv_sem, query_sem, back_sem, before_sem, known_sem,
):
    updated_ref, received_ref = both_ref.at[0], both_ref.at[1]
    key_all, value_all, query_all = (gathered.at[kind] for kind in range(3))
    section = lax.axis_index("section")
    seq = lax.axis_index("seq")
    me = lax.rem(seq, GROUP)
    base = seq - me
    row, side = lax.div(me, 2), lax.rem(me, 2)
    width = gathered.shape[3]
    others = pl.ds(1, GROUP - 1)
    working = (me >= WORKERS[0]) & (me <= WORKERS[-1])
    last = section == sections - 1
    direct = (lax.rem(section, 2) == 0) & jnp.logical_not(last)
    ahead = direct & (me == 0)
    behind = (lax.rem(section, 2) == 1) & (me == 0)

    loads = [
        pltpu.make_async_copy(source, held.at[kind], load_sem.at[0])
        for kind, source in enumerate((key_hbm, value_hbm, query_hbm))
    ]
    for load in loads:
        load.start()

    def here(run):
        for mine in range(GROUP):

            @pl.when(me == mine)
            def _():
                run(mine)

    def signal(sem, place):
        pl.semaphore_signal(sem, inc=1, device_id={"seq": base + place}, device_id_type=MESH)

    barrier = pltpu.get_barrier_semaphore()

    def greet(mine):
        for theirs in range(GROUP):
            later = theirs // 2 > mine // 2 and (mine % 2 == 0 or theirs % 2)
            if later or theirs == mine + 1 - mine % 2 * 2 and (mine % 2 == 0 or mine == 1):
                signal(barrier, theirs)

    here(greet)

    @pl.when(section < sections - 1)
    def _():
        pl.semaphore_signal(barrier, inc=1, device_id={"section": section + 1}, device_id_type=MESH)

    stream_load = pltpu.make_async_copy(stream_hbm, stream_own, load_sem.at[1])
    stream_load.start()

    @pl.when(section == 0)
    def _():
        pltpu.make_async_copy(incoming_hbm, received_ref, recv_sem.at[1]).start()

    def exchange(kind, mine, theirs):
        return pltpu.make_async_remote_copy(
            src_ref=held.at[kind, :, pl.ds((theirs - WORKERS[0]) * width, width)],
            dst_ref=gathered.at[kind, mine ^ theirs],
            send_sem=send_sem.at[3 if kind == 2 else 0],
            recv_sem=query_sem.at[(mine ^ theirs) // 2] if kind == 2 else recv_sem.at[0],
            device_id={"seq": base + theirs},
            device_id_type=MESH,
        )

    def giving_back(mask):
        place = 0
        for weight in (1, 2, 4):
            bit = lax.rem(lax.div(me, weight), 2)
            place = place + weight * ((1 - bit) if mask & weight else bit)
        return pltpu.make_async_remote_copy(
            src_ref=result.at[mask],
            dst_ref=attended.at[me - WORKERS[0]],
            send_sem=send_sem.at[1],
            recv_sem=back_sem.at[me - WORKERS[0]],
            device_id={"seq": base + place},
            device_id_type=MESH,
        )

    def giving_ahead(mask):
        return pltpu.make_async_remote_copy(
            src_ref=result.at[mask],
            dst_ref=attended_before.at[me - WORKERS[0]],
            send_sem=send_sem.at[1],
            recv_sem=before_sem.at[0],
            device_id={"section": lax.rem(section + 1, sections), "seq": base},
            device_id_type=MESH,
        )

    def passing(cols):
        return pltpu.make_async_remote_copy(
            src_ref=updated_ref.at[:, cols],
            dst_ref=received_ref.at[:, cols],
            send_sem=send_sem.at[2],
            recv_sem=recv_sem.at[1],
            device_id={"section": lax.rem(section + 1, sections)},
            device_id_type=MESH,
        )

    def landed(ref, sem):
        pltpu.make_async_copy(ref, ref, sem).wait()

    greeted = jnp.where(side == 0, jnp.maximum(row, 1), 2 * row + 1)
    pl.semaphore_wait(barrier, greeted + jnp.where(section > 0, 1, 0))

    def answer(mine):
        for theirs in range(GROUP):
            if mine in notices(theirs):
                signal(known_sem.at[mine ^ theirs], theirs)

    here(answer)

    @pl.when(section > 0)
    def _():
        pl.semaphore_signal(
            known_sem.at[0], inc=1, device_id={"section": section - 1}, device_id_type=MESH
        )

    landed(held, load_sem.at[0])
    def send(orders, earlier):
        for number, order in enumerate(orders):
            mine, met = number % GROUP, {None}
            for theirs, _ in earlier[number]:
                if theirs is not None:
                    met.add(notice(mine, theirs))
            if order:

                @pl.when(me + GROUP * lax.rem(section, 2) == number)
                def _():
                    for theirs, kinds in order:
                        if theirs is None:
                            pl.delay(kinds)
                            continue
                        shown = notice(mine, theirs)
                        if shown not in met:
                            met.add(shown)
                            pl.semaphore_wait(known_sem.at[mine ^ shown], 1)
                        for kind in kinds:
                            exchange(kind, mine, theirs).start()

    @pl.when(ahead)
    def _():
        pl.semaphore_wait(known_sem.at[0], 1)

    send(SEND_ORDER, [()] * len(SEND_ORDER))

    @pl.when(ahead)
    def _():
        pltpu.make_async_remote_copy(
            src_ref=stream_hbm,
            dst_ref=stream_before,
            send_sem=send_sem.at[2],
            recv_sem=recv_sem.at[1],
            device_id={"section": lax.rem(section + 1, sections)},
            device_id_type=MESH,
        ).start()

    factor = HEAD_SIZE ** -0.5 * LOG2_E

    def attend(pair, count):
        at = pl.ds(2 * pair, 2 * count)
        for start in range(0, width, 2 * HEAD_SIZE):
            heads = [pl.ds(start + offset, HEAD_SIZE) for offset in (0, HEAD_SIZE)]
            scores = [
                lax.dot_general(
                    query_all[at, :, head].reshape(-1, HEAD_SIZE),
                    key_all[:, :, head].reshape(-1, HEAD_SIZE),
                    (((1,), (1,)), ((), ())),
                    preferred_element_type=jnp.float32,
                )
                for head in heads
            ]
            highest = [jnp.max(its, axis=-1, keepdims=True) for its in scores]
            exponent = [jnp.exp2((its - top) * factor) for its, top in zip(scores, highest)]
            totals = [jnp.sum(its, axis=-1, keepdims=True) for its in exponent]
            summed = [
                jnp.dot(
                    its.astype(jnp.bfloat16), value_all[:, :, head].reshape(-1, HEAD_SIZE),
                    preferred_element_type=jnp.float32,
                )
                for its, head in zip(exponent, heads)
            ]
            for its, total, head in zip(summed, totals, heads):
                out = (its * (1.0 / total)).astype(jnp.bfloat16)
                result[at, :, head] = out.reshape(2 * count, -1, HEAD_SIZE)

    @pl.when(working)
    def _():
        own = pl.ds(pl.multiple_of((me - WORKERS[0]) * width, HEAD_SIZE), width)
        for kind in range(3):
            gathered[kind, 0] = held[kind, :, own]
        landed(gathered.at[pl.ds(0, 2), others], recv_sem.at[0])

    @pl.when(jnp.logical_not(working))
    def _():
        landed(held.at[pl.ds(0, 2)], send_sem.at[0])

    send(LATE_ORDER, SEND_ORDER)

    for number, order in enumerate(SERVE_ORDER):

        @pl.when(row == WORKERS[0] // 2 + number)
        def _():
            for pair, count in order:
                for its in range(pair, pair + count):
                    landed(query_all.at[pl.ds(2 * its, 2) if its else pl.ds(1, 1)], query_sem.at[its])
                attend(pair, count)
                for mask in range(2 * pair, 2 * (pair + count)):
                    if mask // 2 == WORKERS[0] // 2 + number:

                        @pl.when(me == mask)
                        def _():
                            giving_back(mask).start()

                            @pl.when(direct)
                            def _():
                                giving_ahead(mask).start()

                for mask in range(2 * pair, 2 * (pair + count)):
                    if mask // 2 == WORKERS[0] // 2 + number:

                        @pl.when(me != mask)
                        def _():
                            giving_back(mask).start()

                    elif mask:
                        giving_back(mask).start()

    landed(stream_own, load_sem.at[1])

    passes = jnp.logical_not(last | ahead)

    @pl.when(passes)
    def _():
        pl.semaphore_wait(known_sem.at[0], 1)

    def plus(stream, piece):
        return (stream.astype(jnp.float32) + piece.astype(jnp.float32)).astype(jnp.bfloat16)

    def finish(worker):
        cols = pl.ds((worker - WORKERS[0]) * width, width)

        def update(piece):
            updated_ref[:, cols] = plus(stream_own[:, cols], piece)

        @pl.when(me == worker)
        def _():
            update(result[0])

        @pl.when(me != worker)
        def _():
            landed(attended.at[worker - WORKERS[0]], back_sem.at[worker - WORKERS[0]])
            update(attended[worker - WORKERS[0]])

        @pl.when(passes)
        def _():
            passing(cols).start()

    for order in sorted(set(FINISH_ORDER)):
        chosen = functools.reduce(
            jnp.logical_or, [row == number for number, its in enumerate(FINISH_ORDER) if its == order]
        )

        @pl.when(chosen)
        def _():
            for worker in order:
                finish(worker)

    @pl.when(working)
    def _():
        most = pl.ds(0, (len(WORKERS) - 1) * width)
        landed(held.at[pl.ds(0, 2), :, most], send_sem.at[0])
        landed(held.at[2, :, most], send_sem.at[3])

        @pl.when(direct)
        def _():
            landed(result, send_sem.at[1])

        @pl.when(jnp.logical_not(direct))
        def _():
            landed(result.at[others], send_sem.at[1])

    @pl.when(jnp.logical_not(working))
    def _():
        landed(held.at[2], send_sem.at[3])

    @pl.when(section < sections - 1)
    def _():
        landed(updated_ref, send_sem.at[2])

    @pl.when(behind)
    def _():
        landed(stream_before, recv_sem.at[1])
        landed(attended_before, before_sem.at[0])
        for worker in WORKERS:
            cols = pl.ds((worker - WORKERS[0]) * width, width)
            received_ref[:, cols] = plus(stream_before[:, cols], attended_before[worker - WORKERS[0]])

    @pl.when(jnp.logical_not(behind))
    def _():
        landed(received_ref, recv_sem.at[1])


def per_device(sections, stream, queries, key_rows, values, incoming):
    rows, features = incoming.shape
    width = features // len(WORKERS)
    both = pl.pallas_call(
        functools.partial(kernel, sections),
        out_shape=pltpu.VMEM((2, rows, features), jnp.bfloat16),
        in_specs=[pl.BlockSpec(memory_space=pl.ANY)] * 5,
        out_specs=pl.BlockSpec(memory_space=pltpu.VMEM),
        scratch_shapes=[
            pltpu.VMEM((rows, features), jnp.bfloat16),
            pltpu.VMEM((3, rows, features), jnp.bfloat16),
            pltpu.VMEM((3, GROUP, rows, width), jnp.bfloat16),
            pltpu.VMEM((GROUP, rows, width), jnp.bfloat16),
            pltpu.VMEM((len(WORKERS), rows, width), jnp.bfloat16),
            pltpu.VMEM((rows, features), jnp.bfloat16),
            pltpu.VMEM((len(WORKERS), rows, width), jnp.bfloat16),
            pltpu.SemaphoreType.DMA((2,)),
            pltpu.SemaphoreType.DMA((4,)),
            pltpu.SemaphoreType.DMA((2,)),
            pltpu.SemaphoreType.DMA((GROUP // 2,)),
            pltpu.SemaphoreType.DMA((len(WORKERS),)),
            pltpu.SemaphoreType.DMA((1,)),
            pltpu.SemaphoreType.REGULAR((GROUP,)),
        ],
        compiler_params=pltpu.CompilerParams(collective_id=0, has_side_effects=True),
    )(stream[0], queries[0], key_rows[0], values[0], incoming)
    return both[:1], both[1:]


def solution(mesh):
    placed = (
        P("section", "seq", None),
        P("section", "seq", None),
        P("section", "seq", None),
        P("section", "seq", None),
        P("seq", None),
    )
    return jax.shard_map(
        functools.partial(per_device, mesh.shape["section"]),
        mesh=mesh,
        in_specs=placed,
        out_specs=(P("section", "seq", None), P("section", "seq", None)),
        check_vma=False,
    )
```

```python
import functools

import jax
import jax.numpy as jnp
from jax import lax
from jax.experimental import pallas as pl
from jax.experimental.pallas import tpu as pltpu
from jax.sharding import PartitionSpec as P

HEAD_SIZE = 128
GROUP = 8
WORKERS = (2, 3, 4, 5)
LOG2_E = 1.4426950408889634
MESH = pl.DeviceIdType.MESH
KEY_VALUE, QUERY, ALL = (0, 1), (2,), (0, 1, 2)
SEND_ORDER = (
    ((2, QUERY), (3, KEY_VALUE), (3, QUERY), (4, QUERY), (5, QUERY), (4, KEY_VALUE), (5, KEY_VALUE), (2, KEY_VALUE)),
    ((3, QUERY), (2, KEY_VALUE), (2, QUERY), (5, QUERY), (4, QUERY), (5, KEY_VALUE), (4, KEY_VALUE), (3, KEY_VALUE)),
    ((4, KEY_VALUE), (5, KEY_VALUE), (3, KEY_VALUE), (4, QUERY), (5, QUERY), (3, QUERY)),
    ((5, KEY_VALUE), (4, KEY_VALUE), (2, KEY_VALUE), (5, QUERY), (4, QUERY), (2, QUERY)),
    ((2, KEY_VALUE), (3, KEY_VALUE), (5, KEY_VALUE), (2, QUERY), (3, QUERY), (5, QUERY)),
    ((3, KEY_VALUE), (2, KEY_VALUE), (4, KEY_VALUE), (3, QUERY), (2, QUERY), (4, QUERY)),
    ((2, KEY_VALUE), (3, KEY_VALUE), (4, KEY_VALUE), (5, KEY_VALUE), (2, QUERY), (3, QUERY), (4, QUERY), (5, QUERY)),
    ((3, KEY_VALUE), (2, KEY_VALUE), (5, KEY_VALUE), (4, KEY_VALUE), (3, QUERY), (2, QUERY), (5, QUERY), (4, QUERY)),
    ((None, 500), (2, KEY_VALUE), (3, KEY_VALUE), (4, KEY_VALUE), (5, KEY_VALUE), (4, QUERY), (5, QUERY), (2, QUERY), (3, QUERY)),
    ((None, 500), (3, KEY_VALUE), (2, KEY_VALUE), (5, KEY_VALUE), (4, KEY_VALUE), (5, QUERY), (4, QUERY), (3, QUERY), (2, QUERY)),
    ((None, 500), (4, KEY_VALUE), (5, KEY_VALUE), (3, KEY_VALUE), (4, QUERY), (5, QUERY), (3, QUERY)),
    ((None, 500), (5, KEY_VALUE), (4, KEY_VALUE), (2, KEY_VALUE), (5, QUERY), (4, QUERY), (2, QUERY)),
    ((None, 500), (2, KEY_VALUE), (3, KEY_VALUE), (5, KEY_VALUE), (2, QUERY), (3, QUERY), (5, QUERY)),
    ((None, 500), (3, KEY_VALUE), (2, KEY_VALUE), (4, KEY_VALUE), (3, QUERY), (2, QUERY), (4, QUERY)),
    ((None, 500), (2, KEY_VALUE), (3, KEY_VALUE), (4, KEY_VALUE), (5, KEY_VALUE), (2, QUERY), (3, QUERY), (4, QUERY), (5, QUERY)),
    ((None, 500), (3, KEY_VALUE), (2, KEY_VALUE), (5, KEY_VALUE), (4, KEY_VALUE), (3, QUERY), (2, QUERY), (5, QUERY), (4, QUERY)),
)
LATE_ORDER = (
    (),
    (),
    (),
    (),
    (),
    (),
    (),
    (),
    (),
    (),
    (),
    (),
    (),
    (),
    (),
    (),
)
SERVE_ORDER = (((1, 1), (3, 1), (2, 1), (0, 1)), ((2, 1), (3, 1), (0, 1), (1, 1)))
FINISH_ORDER = ((2, 3, 4, 5), (2, 3, 4, 5), (2, 3, 4, 5), (2, 3, 4, 5))


def notice(mine, theirs):
    if theirs // 2 > mine // 2:
        return theirs if mine % 2 == 0 else theirs | 1
    if mine % 2 == 0 and theirs % 2 and mine > 0:
        return mine + 1
    return None


def notices(mine):
    return {notice(mine, theirs) for theirs in WORKERS if theirs != mine} - {None}


def kernel(
    sections,
    stream_hbm, query_hbm, key_hbm, value_hbm, incoming_hbm,
    both_ref,
    stream_own, held, gathered, result, attended, stream_before, attended_before,
    load_sem, send_sem, recv_sem, query_sem, back_sem, before_sem, known_sem,
):
    updated_ref, received_ref = both_ref.at[0], both_ref.at[1]
    key_all, value_all, query_all = (gathered.at[kind] for kind in range(3))
    section = lax.axis_index("section")
    seq = lax.axis_index("seq")
    me = lax.rem(seq, GROUP)
    base = seq - me
    row, side = lax.div(me, 2), lax.rem(me, 2)
    width = gathered.shape[3]
    others = pl.ds(1, GROUP - 1)
    working = (me >= WORKERS[0]) & (me <= WORKERS[-1])
    last = section == sections - 1
    direct = (lax.rem(section, 2) == 0) & jnp.logical_not(last)
    behind = lax.rem(section, 2) == 1

    loads = [
        pltpu.make_async_copy(source, held.at[kind], load_sem.at[0])
        for kind, source in enumerate((key_hbm, value_hbm, query_hbm))
    ]
    for load in loads:
        load.start()

    def here(run):
        for mine in range(GROUP):

            @pl.when(me == mine)
            def _():
                run(mine)

    def signal(sem, place):
        pl.semaphore_signal(sem, inc=1, device_id={"seq": base + place}, device_id_type=MESH)

    barrier = pltpu.get_barrier_semaphore()

    def greet(mine):
        for theirs in range(GROUP):
            later = theirs // 2 > mine // 2 and (mine % 2 == 0 or theirs % 2)
            if later or theirs == mine + 1 - mine % 2 * 2 and (mine % 2 == 0 or mine == 1):
                signal(barrier, theirs)

    here(greet)

    @pl.when(section < sections - 1)
    def _():
        pl.semaphore_signal(barrier, inc=1, device_id={"section": section + 1}, device_id_type=MESH)

    stream_load = pltpu.make_async_copy(stream_hbm, stream_own, load_sem.at[1])
    stream_load.start()

    @pl.when(section == 0)
    def _():
        pltpu.make_async_copy(incoming_hbm, received_ref, recv_sem.at[1]).start()

    def exchange(kind, mine, theirs):
        return pltpu.make_async_remote_copy(
            src_ref=held.at[kind, :, pl.ds((theirs - WORKERS[0]) * width, width)],
            dst_ref=gathered.at[kind, mine ^ theirs],
            send_sem=send_sem.at[3 if kind == 2 else 0],
            recv_sem=query_sem.at[(mine ^ theirs) // 2] if kind == 2 else recv_sem.at[0],
            device_id={"seq": base + theirs},
            device_id_type=MESH,
        )

    def place_at(mask):
        place = 0
        for weight in (1, 2, 4):
            bit = lax.rem(lax.div(me, weight), 2)
            place = place + weight * ((1 - bit) if mask & weight else bit)
        return place

    def giving_back(mask):
        return pltpu.make_async_remote_copy(
            src_ref=result.at[mask],
            dst_ref=attended.at[me - WORKERS[0]],
            send_sem=send_sem.at[1],
            recv_sem=back_sem.at[me - WORKERS[0]],
            device_id={"seq": base + place_at(mask)},
            device_id_type=MESH,
        )

    def giving_ahead(mask):
        return pltpu.make_async_remote_copy(
            src_ref=result.at[mask],
            dst_ref=attended_before.at[me - WORKERS[0]],
            send_sem=send_sem.at[1 if mask else 4],
            recv_sem=before_sem.at[me - WORKERS[0]],
            device_id={"section": lax.rem(section + 1, sections), "seq": base + place_at(mask)},
            device_id_type=MESH,
        )

    def give(mask):
        if mask:

            @pl.when(jnp.logical_not(direct) | (me == mask))
            def _():
                giving_back(mask).start()

        @pl.when(direct)
        def _():
            giving_ahead(mask).start()

    def handing_on(worker):
        index = worker - WORKERS[0]
        return pltpu.make_async_remote_copy(
            src_ref=attended_before.at[index],
            dst_ref=attended.at[index],
            send_sem=send_sem.at[4],
            recv_sem=back_sem.at[index],
            device_id={"section": lax.rem(section + sections - 1, sections)},
            device_id_type=MESH,
        )

    def passing(cols):
        return pltpu.make_async_remote_copy(
            src_ref=updated_ref.at[:, cols],
            dst_ref=received_ref.at[:, cols],
            send_sem=send_sem.at[2],
            recv_sem=recv_sem.at[1],
            device_id={"section": lax.rem(section + 1, sections)},
            device_id_type=MESH,
        )

    def landed(ref, sem):
        pltpu.make_async_copy(ref, ref, sem).wait()

    greeted = jnp.where(side == 0, jnp.maximum(row, 1), 2 * row + 1)
    pl.semaphore_wait(barrier, greeted + jnp.where(section > 0, 1, 0))

    def answer(mine):
        for theirs in range(GROUP):
            if mine in notices(theirs):
                signal(known_sem.at[mine ^ theirs], theirs)

    here(answer)

    @pl.when(section > 0)
    def _():
        pl.semaphore_signal(
            known_sem.at[0], inc=1, device_id={"section": section - 1}, device_id_type=MESH
        )

    landed(held, load_sem.at[0])
    def send(orders, earlier):
        for number, order in enumerate(orders):
            mine, met = number % GROUP, {None}
            for theirs, _ in earlier[number]:
                if theirs is not None:
                    met.add(notice(mine, theirs))
            if order:

                @pl.when(me + GROUP * lax.rem(section, 2) == number)
                def _():
                    for theirs, kinds in order:
                        if theirs is None:
                            pl.delay(kinds)
                            continue
                        shown = notice(mine, theirs)
                        if shown not in met:
                            met.add(shown)
                            pl.semaphore_wait(known_sem.at[mine ^ shown], 1)
                        for kind in kinds:
                            exchange(kind, mine, theirs).start()

    @pl.when(direct)
    def _():
        pl.semaphore_wait(known_sem.at[0], 1)

    send(SEND_ORDER, [()] * len(SEND_ORDER))

    @pl.when(direct)
    def _():
        pltpu.make_async_remote_copy(
            src_ref=stream_hbm,
            dst_ref=stream_before,
            send_sem=send_sem.at[2],
            recv_sem=recv_sem.at[1],
            device_id={"section": lax.rem(section + 1, sections)},
            device_id_type=MESH,
        ).start()

    factor = HEAD_SIZE ** -0.5 * LOG2_E

    def attend(pair, count):
        at = pl.ds(2 * pair, 2 * count)
        for start in range(0, width, 2 * HEAD_SIZE):
            heads = [pl.ds(start + offset, HEAD_SIZE) for offset in (0, HEAD_SIZE)]
            scores = [
                lax.dot_general(
                    query_all[at, :, head].reshape(-1, HEAD_SIZE),
                    key_all[:, :, head].reshape(-1, HEAD_SIZE),
                    (((1,), (1,)), ((), ())),
                    preferred_element_type=jnp.float32,
                )
                for head in heads
            ]
            highest = [jnp.max(its, axis=-1, keepdims=True) for its in scores]
            exponent = [jnp.exp2((its - top) * factor) for its, top in zip(scores, highest)]
            totals = [jnp.sum(its, axis=-1, keepdims=True) for its in exponent]
            summed = [
                jnp.dot(
                    its.astype(jnp.bfloat16), value_all[:, :, head].reshape(-1, HEAD_SIZE),
                    preferred_element_type=jnp.float32,
                )
                for its, head in zip(exponent, heads)
            ]
            for its, total, head in zip(summed, totals, heads):
                out = (its * (1.0 / total)).astype(jnp.bfloat16)
                result[at, :, head] = out.reshape(2 * count, -1, HEAD_SIZE)

    @pl.when(working)
    def _():
        own = pl.ds(pl.multiple_of((me - WORKERS[0]) * width, HEAD_SIZE), width)
        for kind in range(3):
            gathered[kind, 0] = held[kind, :, own]
        landed(gathered.at[pl.ds(0, 2), others], recv_sem.at[0])

    @pl.when(jnp.logical_not(working))
    def _():
        landed(held.at[pl.ds(0, 2)], send_sem.at[0])

    send(LATE_ORDER, SEND_ORDER)

    for number, order in enumerate(SERVE_ORDER):

        @pl.when(row == WORKERS[0] // 2 + number)
        def _():
            for pair, count in order:
                for its in range(pair, pair + count):
                    landed(query_all.at[pl.ds(2 * its, 2) if its else pl.ds(1, 1)], query_sem.at[its])
                attend(pair, count)
                masks = range(2 * pair, 2 * (pair + count))
                for mask in masks:

                    @pl.when(me == mask)
                    def _():
                        give(mask)

                for mask in masks:

                    @pl.when(me != mask)
                    def _():
                        give(mask)

    landed(stream_own, load_sem.at[1])

    passes = jnp.logical_not(last | direct)

    @pl.when(passes)
    def _():
        pl.semaphore_wait(known_sem.at[0], 1)

    def plus(stream, piece):
        return (stream.astype(jnp.float32) + piece.astype(jnp.float32)).astype(jnp.bfloat16)

    def finish(worker):
        cols = pl.ds((worker - WORKERS[0]) * width, width)

        def update(piece):
            updated_ref[:, cols] = plus(stream_own[:, cols], piece)

        @pl.when(me == worker)
        def _():
            update(result[0])

        @pl.when(me != worker)
        def _():
            landed(attended.at[worker - WORKERS[0]], back_sem.at[worker - WORKERS[0]])
            update(attended[worker - WORKERS[0]])

        @pl.when(passes)
        def _():
            passing(cols).start()

    for order in sorted(set(FINISH_ORDER)):
        chosen = functools.reduce(
            jnp.logical_or, [row == number for number, its in enumerate(FINISH_ORDER) if its == order]
        )

        @pl.when(chosen)
        def _():
            for worker in order:
                finish(worker)

    @pl.when(behind)
    def _():
        landed(stream_before, recv_sem.at[1])
        for worker in (2, 3, 4, 5):
            index = worker - WORKERS[0]
            landed(attended_before.at[index], before_sem.at[index])

            @pl.when((me > 0) & (me != worker))
            def _():
                handing_on(worker).start()

            cols = pl.ds(index * width, width)
            received_ref[:, cols] = plus(stream_before[:, cols], attended_before[index])

        @pl.when(working)
        def _():
            landed(attended_before.at[pl.ds(1, len(WORKERS) - 1)], send_sem.at[4])

        @pl.when((me > 0) & jnp.logical_not(working))
        def _():
            landed(attended_before, send_sem.at[4])

    @pl.when(working)
    def _():
        most = pl.ds(0, (len(WORKERS) - 1) * width)
        landed(held.at[pl.ds(0, 2), :, most], send_sem.at[0])
        landed(held.at[2, :, most], send_sem.at[3])

        @pl.when(direct)
        def _():
            landed(result, send_sem.at[1])
            landed(result.at[0], send_sem.at[4])

        @pl.when(jnp.logical_not(direct))
        def _():
            landed(result.at[others], send_sem.at[1])

    @pl.when(jnp.logical_not(working))
    def _():
        landed(held.at[2], send_sem.at[3])

    @pl.when(section < sections - 1)
    def _():
        landed(updated_ref, send_sem.at[2])

    @pl.when(jnp.logical_not(behind))
    def _():
        landed(received_ref, recv_sem.at[1])


def per_device(sections, stream, queries, key_rows, values, incoming):
    rows, features = incoming.shape
    width = features // len(WORKERS)
    both = pl.pallas_call(
        functools.partial(kernel, sections),
        out_shape=pltpu.VMEM((2, rows, features), jnp.bfloat16),
        in_specs=[pl.BlockSpec(memory_space=pl.ANY)] * 5,
        out_specs=pl.BlockSpec(memory_space=pltpu.VMEM),
        scratch_shapes=[
            pltpu.VMEM((rows, features), jnp.bfloat16),
            pltpu.VMEM((3, rows, features), jnp.bfloat16),
            pltpu.VMEM((3, GROUP, rows, width), jnp.bfloat16),
            pltpu.VMEM((GROUP, rows, width), jnp.bfloat16),
            pltpu.VMEM((len(WORKERS), rows, width), jnp.bfloat16),
            pltpu.VMEM((rows, features), jnp.bfloat16),
            pltpu.VMEM((len(WORKERS), rows, width), jnp.bfloat16),
            pltpu.SemaphoreType.DMA((2,)),
            pltpu.SemaphoreType.DMA((5,)),
            pltpu.SemaphoreType.DMA((2,)),
            pltpu.SemaphoreType.DMA((GROUP // 2,)),
            pltpu.SemaphoreType.DMA((len(WORKERS),)),
            pltpu.SemaphoreType.DMA((len(WORKERS),)),
            pltpu.SemaphoreType.REGULAR((GROUP,)),
        ],
        compiler_params=pltpu.CompilerParams(collective_id=0, has_side_effects=True),
    )(stream[0], queries[0], key_rows[0], values[0], incoming)
    return both[:1], both[1:]


def solution(mesh):
    placed = (
        P("section", "seq", None),
        P("section", "seq", None),
        P("section", "seq", None),
        P("section", "seq", None),
        P("seq", None),
    )
    return jax.shard_map(
        functools.partial(per_device, mesh.shape["section"]),
        mesh=mesh,
        in_specs=placed,
        out_specs=(P("section", "seq", None), P("section", "seq", None)),
        check_vma=False,
    )
```

```python
import functools

import jax
import jax.numpy as jnp
from jax import lax
from jax.experimental import pallas as pl
from jax.experimental.pallas import tpu as pltpu
from jax.sharding import PartitionSpec as P

HEAD_SIZE = 128
GROUP = 8
WORKERS = (2, 3, 4, 5)
LOG2_E = 1.4426950408889634
MESH = pl.DeviceIdType.MESH
KEY_VALUE, QUERY, ALL = (0, 1), (2,), (0, 1, 2)
SEND_ORDER = (
    ((2, QUERY), (3, KEY_VALUE), (4, QUERY), (5, QUERY), (3, QUERY), (4, KEY_VALUE), (5, KEY_VALUE), (2, KEY_VALUE)),
    ((3, QUERY), (2, KEY_VALUE), (5, QUERY), (4, QUERY), (2, QUERY), (5, KEY_VALUE), (4, KEY_VALUE), (3, KEY_VALUE)),
    ((4, KEY_VALUE), (5, KEY_VALUE), (3, KEY_VALUE), (4, QUERY), (5, QUERY), (3, QUERY)),
    ((5, KEY_VALUE), (4, KEY_VALUE), (2, KEY_VALUE), (5, QUERY), (4, QUERY), (2, QUERY)),
    ((2, KEY_VALUE), (3, KEY_VALUE), (5, KEY_VALUE), (2, QUERY), (3, QUERY), (5, QUERY)),
    ((3, KEY_VALUE), (2, KEY_VALUE), (4, KEY_VALUE), (3, QUERY), (2, QUERY), (4, QUERY)),
    ((2, KEY_VALUE), (3, KEY_VALUE), (4, KEY_VALUE), (5, KEY_VALUE), (2, QUERY), (3, QUERY), (4, QUERY), (5, QUERY)),
    ((3, KEY_VALUE), (2, KEY_VALUE), (5, KEY_VALUE), (4, KEY_VALUE), (3, QUERY), (2, QUERY), (5, QUERY), (4, QUERY)),
    ((None, 500), (2, KEY_VALUE), (3, KEY_VALUE), (4, KEY_VALUE), (5, KEY_VALUE), (4, QUERY), (5, QUERY), (2, QUERY), (3, QUERY)),
    ((None, 500), (3, KEY_VALUE), (2, KEY_VALUE), (5, KEY_VALUE), (4, KEY_VALUE), (5, QUERY), (4, QUERY), (3, QUERY), (2, QUERY)),
    ((None, 500), (4, KEY_VALUE), (5, KEY_VALUE), (3, KEY_VALUE), (4, QUERY), (5, QUERY), (3, QUERY)),
    ((None, 500), (5, KEY_VALUE), (4, KEY_VALUE), (2, KEY_VALUE), (5, QUERY), (4, QUERY), (2, QUERY)),
    ((None, 500), (2, KEY_VALUE), (3, KEY_VALUE), (5, KEY_VALUE), (2, QUERY), (3, QUERY), (5, QUERY)),
    ((None, 500), (3, KEY_VALUE), (2, KEY_VALUE), (4, KEY_VALUE), (3, QUERY), (2, QUERY), (4, QUERY)),
    ((None, 500), (2, KEY_VALUE), (3, KEY_VALUE), (4, KEY_VALUE), (5, KEY_VALUE), (2, QUERY), (3, QUERY), (4, QUERY), (5, QUERY)),
    ((None, 500), (3, KEY_VALUE), (2, KEY_VALUE), (5, KEY_VALUE), (4, KEY_VALUE), (3, QUERY), (2, QUERY), (5, QUERY), (4, QUERY)),
)
LATE_ORDER = (
    (),
    (),
    (),
    (),
    (),
    (),
    (),
    (),
    (),
    (),
    (),
    (),
    (),
    (),
    (),
    (),
)
SERVE_ORDER = (((1, 1), (3, 1), (2, 1), (0, 1)), ((2, 1), (0, 1), (3, 1), (1, 1)))
FINISH_ORDER = ((2, 3, 4, 5), (2, 3, 4, 5), (2, 3, 4, 5), (2, 3, 4, 5))


def notice(mine, theirs):
    if theirs // 2 > mine // 2:
        return theirs if mine % 2 == 0 else theirs | 1
    if mine % 2 == 0 and theirs % 2 and mine > 0:
        return mine + 1
    return None


def notices(mine):
    return {notice(mine, theirs) for theirs in WORKERS if theirs != mine} - {None}


def kernel(
    sections,
    stream_hbm, query_hbm, key_hbm, value_hbm, incoming_hbm,
    both_ref,
    stream_own, held, gathered, result, attended, stream_before, attended_before,
    load_sem, send_sem, recv_sem, query_sem, back_sem, before_sem, known_sem,
):
    updated_ref, received_ref = both_ref.at[0], both_ref.at[1]
    key_all, value_all, query_all = (gathered.at[kind] for kind in range(3))
    section = lax.axis_index("section")
    seq = lax.axis_index("seq")
    me = lax.rem(seq, GROUP)
    base = seq - me
    row, side = lax.div(me, 2), lax.rem(me, 2)
    width = gathered.shape[3]
    others = pl.ds(1, GROUP - 1)
    working = (me >= WORKERS[0]) & (me <= WORKERS[-1])
    last = section == sections - 1
    direct = (lax.rem(section, 2) == 0) & jnp.logical_not(last)
    behind = lax.rem(section, 2) == 1

    loads = [
        pltpu.make_async_copy(source, held.at[kind], load_sem.at[0])
        for kind, source in enumerate((key_hbm, value_hbm, query_hbm))
    ]
    for load in loads:
        load.start()

    def here(run):
        for mine in range(GROUP):

            @pl.when(me == mine)
            def _():
                run(mine)

    def signal(sem, place):
        pl.semaphore_signal(sem, inc=1, device_id={"seq": base + place}, device_id_type=MESH)

    barrier = pltpu.get_barrier_semaphore()

    def greet(mine):
        for theirs in range(GROUP):
            later = theirs // 2 > mine // 2 and (mine % 2 == 0 or theirs % 2)
            if later or theirs == mine + 1 - mine % 2 * 2 and (mine % 2 == 0 or mine == 1):
                signal(barrier, theirs)

    here(greet)

    @pl.when(section < sections - 1)
    def _():
        pl.semaphore_signal(barrier, inc=1, device_id={"section": section + 1}, device_id_type=MESH)

    stream_load = pltpu.make_async_copy(stream_hbm, stream_own, load_sem.at[1])
    stream_load.start()

    @pl.when(section == 0)
    def _():
        pltpu.make_async_copy(incoming_hbm, received_ref, recv_sem.at[1]).start()

    def exchange(kind, mine, theirs):
        return pltpu.make_async_remote_copy(
            src_ref=held.at[kind, :, pl.ds((theirs - WORKERS[0]) * width, width)],
            dst_ref=gathered.at[kind, mine ^ theirs],
            send_sem=send_sem.at[3 if kind == 2 else 0],
            recv_sem=query_sem.at[(mine ^ theirs) // 2] if kind == 2 else recv_sem.at[0],
            device_id={"seq": base + theirs},
            device_id_type=MESH,
        )

    def place_at(mask):
        place = 0
        for weight in (1, 2, 4):
            bit = lax.rem(lax.div(me, weight), 2)
            place = place + weight * ((1 - bit) if mask & weight else bit)
        return place

    def giving_back(mask):
        return pltpu.make_async_remote_copy(
            src_ref=result.at[mask],
            dst_ref=attended.at[me - WORKERS[0]],
            send_sem=send_sem.at[1],
            recv_sem=back_sem.at[me - WORKERS[0]],
            device_id={"seq": base + place_at(mask)},
            device_id_type=MESH,
        )

    def giving_ahead(mask):
        return pltpu.make_async_remote_copy(
            src_ref=result.at[mask],
            dst_ref=attended_before.at[me - WORKERS[0]],
            send_sem=send_sem.at[1 if mask else 4],
            recv_sem=before_sem.at[me - WORKERS[0]],
            device_id={"section": lax.rem(section + 1, sections), "seq": base + place_at(mask)},
            device_id_type=MESH,
        )

    def give(mask):
        if mask:

            @pl.when(jnp.logical_not(direct) | (me == mask))
            def _():
                giving_back(mask).start()

        @pl.when(direct)
        def _():
            giving_ahead(mask).start()

    def handing_on(worker):
        index = worker - WORKERS[0]
        return pltpu.make_async_remote_copy(
            src_ref=attended_before.at[index],
            dst_ref=attended.at[index],
            send_sem=send_sem.at[4],
            recv_sem=back_sem.at[index],
            device_id={"section": lax.rem(section + sections - 1, sections)},
            device_id_type=MESH,
        )

    def passing(cols):
        return pltpu.make_async_remote_copy(
            src_ref=updated_ref.at[:, cols],
            dst_ref=received_ref.at[:, cols],
            send_sem=send_sem.at[2],
            recv_sem=recv_sem.at[1],
            device_id={"section": lax.rem(section + 1, sections)},
            device_id_type=MESH,
        )

    def landed(ref, sem):
        pltpu.make_async_copy(ref, ref, sem).wait()

    greeted = jnp.where(side == 0, jnp.maximum(row, 1), 2 * row + 1)
    pl.semaphore_wait(barrier, greeted + jnp.where(section > 0, 1, 0))

    def answer(mine):
        for theirs in range(GROUP):
            if mine in notices(theirs):
                signal(known_sem.at[mine ^ theirs], theirs)

    here(answer)

    @pl.when(section > 0)
    def _():
        pl.semaphore_signal(
            known_sem.at[0], inc=1, device_id={"section": section - 1}, device_id_type=MESH
        )

    landed(held, load_sem.at[0])
    def send(orders, earlier):
        for number, order in enumerate(orders):
            mine, met = number % GROUP, {None}
            for theirs, _ in earlier[number]:
                if theirs is not None:
                    met.add(notice(mine, theirs))
            if order:

                @pl.when(me + GROUP * lax.rem(section, 2) == number)
                def _():
                    for theirs, kinds in order:
                        if theirs is None:
                            pl.delay(kinds)
                            continue
                        shown = notice(mine, theirs)
                        if shown not in met:
                            met.add(shown)
                            pl.semaphore_wait(known_sem.at[mine ^ shown], 1)
                        for kind in kinds:
                            exchange(kind, mine, theirs).start()

    @pl.when(direct)
    def _():
        pl.semaphore_wait(known_sem.at[0], 1)

    send(SEND_ORDER, [()] * len(SEND_ORDER))

    @pl.when(direct)
    def _():
        pltpu.make_async_remote_copy(
            src_ref=stream_hbm,
            dst_ref=stream_before,
            send_sem=send_sem.at[2],
            recv_sem=recv_sem.at[1],
            device_id={"section": lax.rem(section + 1, sections)},
            device_id_type=MESH,
        ).start()

    factor = HEAD_SIZE ** -0.5 * LOG2_E

    def attend(pair, count):
        at = pl.ds(2 * pair, 2 * count)
        for start in range(0, width, 2 * HEAD_SIZE):
            heads = [pl.ds(start + offset, HEAD_SIZE) for offset in (0, HEAD_SIZE)]
            scores = [
                lax.dot_general(
                    query_all[at, :, head].reshape(-1, HEAD_SIZE),
                    key_all[:, :, head].reshape(-1, HEAD_SIZE),
                    (((1,), (1,)), ((), ())),
                    preferred_element_type=jnp.float32,
                )
                for head in heads
            ]
            highest = [jnp.max(its, axis=-1, keepdims=True) for its in scores]
            exponent = [jnp.exp2((its - top) * factor) for its, top in zip(scores, highest)]
            totals = [jnp.sum(its, axis=-1, keepdims=True) for its in exponent]
            summed = [
                jnp.dot(
                    its.astype(jnp.bfloat16), value_all[:, :, head].reshape(-1, HEAD_SIZE),
                    preferred_element_type=jnp.float32,
                )
                for its, head in zip(exponent, heads)
            ]
            for its, total, head in zip(summed, totals, heads):
                out = (its * (1.0 / total)).astype(jnp.bfloat16)
                result[at, :, head] = out.reshape(2 * count, -1, HEAD_SIZE)

    @pl.when(working)
    def _():
        own = pl.ds(pl.multiple_of((me - WORKERS[0]) * width, HEAD_SIZE), width)
        for kind in range(3):
            gathered[kind, 0] = held[kind, :, own]
        landed(gathered.at[pl.ds(0, 2), others], recv_sem.at[0])

    @pl.when(jnp.logical_not(working))
    def _():
        landed(held.at[pl.ds(0, 2)], send_sem.at[0])

    send(LATE_ORDER, SEND_ORDER)

    for number, order in enumerate(SERVE_ORDER):

        @pl.when(row == WORKERS[0] // 2 + number)
        def _():
            for pair, count in order:
                for its in range(pair, pair + count):
                    landed(query_all.at[pl.ds(2 * its, 2) if its else pl.ds(1, 1)], query_sem.at[its])
                attend(pair, count)
                masks = range(2 * pair, 2 * (pair + count))
                for mask in masks:

                    @pl.when(me == mask)
                    def _():
                        give(mask)

                for mask in masks:

                    @pl.when(me != mask)
                    def _():
                        give(mask)

    landed(stream_own, load_sem.at[1])

    passes = jnp.logical_not(last | direct)

    @pl.when(passes)
    def _():
        pl.semaphore_wait(known_sem.at[0], 1)

    def plus(stream, piece):
        return (stream.astype(jnp.float32) + piece.astype(jnp.float32)).astype(jnp.bfloat16)

    def finish(worker):
        cols = pl.ds((worker - WORKERS[0]) * width, width)

        def update(piece):
            updated_ref[:, cols] = plus(stream_own[:, cols], piece)

        @pl.when(me == worker)
        def _():
            update(result[0])

        @pl.when(me != worker)
        def _():
            landed(attended.at[worker - WORKERS[0]], back_sem.at[worker - WORKERS[0]])
            update(attended[worker - WORKERS[0]])

        @pl.when(passes)
        def _():
            passing(cols).start()

    for order in sorted(set(FINISH_ORDER)):
        chosen = functools.reduce(
            jnp.logical_or, [row == number for number, its in enumerate(FINISH_ORDER) if its == order]
        )

        @pl.when(chosen)
        def _():
            for worker in order:
                finish(worker)

    @pl.when(behind)
    def _():
        landed(stream_before, recv_sem.at[1])
        for worker in (2, 3, 4, 5):
            index = worker - WORKERS[0]
            landed(attended_before.at[index], before_sem.at[index])

            @pl.when((me > 0) & (me != worker))
            def _():
                handing_on(worker).start()

            cols = pl.ds(index * width, width)
            received_ref[:, cols] = plus(stream_before[:, cols], attended_before[index])

        @pl.when(working)
        def _():
            landed(attended_before.at[pl.ds(1, len(WORKERS) - 1)], send_sem.at[4])

        @pl.when((me > 0) & jnp.logical_not(working))
        def _():
            landed(attended_before, send_sem.at[4])

    @pl.when(working)
    def _():
        most = pl.ds(0, (len(WORKERS) - 1) * width)
        landed(held.at[pl.ds(0, 2), :, most], send_sem.at[0])
        landed(held.at[2, :, most], send_sem.at[3])

        @pl.when(direct)
        def _():
            landed(result, send_sem.at[1])
            landed(result.at[0], send_sem.at[4])

        @pl.when(jnp.logical_not(direct))
        def _():
            landed(result.at[others], send_sem.at[1])

    @pl.when(jnp.logical_not(working))
    def _():
        landed(held.at[2], send_sem.at[3])

    @pl.when(section < sections - 1)
    def _():
        landed(updated_ref, send_sem.at[2])

    @pl.when(jnp.logical_not(behind))
    def _():
        landed(received_ref, recv_sem.at[1])


def per_device(sections, stream, queries, key_rows, values, incoming):
    rows, features = incoming.shape
    width = features // len(WORKERS)
    both = pl.pallas_call(
        functools.partial(kernel, sections),
        out_shape=pltpu.VMEM((2, rows, features), jnp.bfloat16),
        in_specs=[pl.BlockSpec(memory_space=pl.ANY)] * 5,
        out_specs=pl.BlockSpec(memory_space=pltpu.VMEM),
        scratch_shapes=[
            pltpu.VMEM((rows, features), jnp.bfloat16),
            pltpu.VMEM((3, rows, features), jnp.bfloat16),
            pltpu.VMEM((3, GROUP, rows, width), jnp.bfloat16),
            pltpu.VMEM((GROUP, rows, width), jnp.bfloat16),
            pltpu.VMEM((len(WORKERS), rows, width), jnp.bfloat16),
            pltpu.VMEM((rows, features), jnp.bfloat16),
            pltpu.VMEM((len(WORKERS), rows, width), jnp.bfloat16),
            pltpu.SemaphoreType.DMA((2,)),
            pltpu.SemaphoreType.DMA((5,)),
            pltpu.SemaphoreType.DMA((2,)),
            pltpu.SemaphoreType.DMA((GROUP // 2,)),
            pltpu.SemaphoreType.DMA((len(WORKERS),)),
            pltpu.SemaphoreType.DMA((len(WORKERS),)),
            pltpu.SemaphoreType.REGULAR((GROUP,)),
        ],
        compiler_params=pltpu.CompilerParams(collective_id=0, has_side_effects=True),
    )(stream[0], queries[0], key_rows[0], values[0], incoming)
    return both[:1], both[1:]


def solution(mesh):
    placed = (
        P("section", "seq", None),
        P("section", "seq", None),
        P("section", "seq", None),
        P("section", "seq", None),
        P("seq", None),
    )
    return jax.shard_map(
        functools.partial(per_device, mesh.shape["section"]),
        mesh=mesh,
        in_specs=placed,
        out_specs=(P("section", "seq", None), P("section", "seq", None)),
        check_vma=False,
    )
```

```python
import functools

import jax
import jax.numpy as jnp
from jax import lax
from jax.experimental import pallas as pl
from jax.experimental.pallas import tpu as pltpu
from jax.sharding import PartitionSpec as P

HEAD_SIZE = 128
GROUP = 8
WORKERS = (2, 3, 4, 5)
LOG2_E = 1.4426950408889634
MESH = pl.DeviceIdType.MESH
KEY_VALUE, QUERY, ALL = (0, 1), (2,), (0, 1, 2)
SEND_ORDER = (
    ((2, QUERY), (3, KEY_VALUE), (4, QUERY), (5, QUERY), (3, QUERY), (4, KEY_VALUE), (5, KEY_VALUE), (2, KEY_VALUE)),
    ((3, QUERY), (2, KEY_VALUE), (5, QUERY), (4, QUERY), (2, QUERY), (5, KEY_VALUE), (4, KEY_VALUE), (3, KEY_VALUE)),
    ((4, KEY_VALUE), (5, KEY_VALUE), (3, KEY_VALUE), (3, QUERY), (4, QUERY), (5, QUERY)),
    ((5, KEY_VALUE), (4, KEY_VALUE), (2, KEY_VALUE), (2, QUERY), (5, QUERY), (4, QUERY)),
    ((2, KEY_VALUE), (3, KEY_VALUE), (5, KEY_VALUE), (2, QUERY), (3, QUERY), (5, QUERY)),
    ((3, KEY_VALUE), (2, KEY_VALUE), (4, KEY_VALUE), (3, QUERY), (2, QUERY), (4, QUERY)),
    ((2, KEY_VALUE), (3, KEY_VALUE), (4, KEY_VALUE), (5, KEY_VALUE), (2, QUERY), (3, QUERY), (4, QUERY), (5, QUERY)),
    ((3, KEY_VALUE), (2, KEY_VALUE), (5, KEY_VALUE), (4, KEY_VALUE), (3, QUERY), (2, QUERY), (5, QUERY), (4, QUERY)),
    ((None, 500), (2, KEY_VALUE), (3, KEY_VALUE), (4, KEY_VALUE), (5, KEY_VALUE), (4, QUERY), (5, QUERY), (2, QUERY), (3, QUERY)),
    ((None, 500), (3, KEY_VALUE), (2, KEY_VALUE), (5, KEY_VALUE), (4, KEY_VALUE), (5, QUERY), (4, QUERY), (3, QUERY), (2, QUERY)),
    ((None, 500), (4, KEY_VALUE), (5, KEY_VALUE), (3, KEY_VALUE), (3, QUERY), (4, QUERY), (5, QUERY)),
    ((None, 500), (5, KEY_VALUE), (4, KEY_VALUE), (2, KEY_VALUE), (2, QUERY), (5, QUERY), (4, QUERY)),
    ((None, 500), (2, KEY_VALUE), (3, KEY_VALUE), (5, KEY_VALUE), (2, QUERY), (3, QUERY), (5, QUERY)),
    ((None, 500), (3, KEY_VALUE), (2, KEY_VALUE), (4, KEY_VALUE), (3, QUERY), (2, QUERY), (4, QUERY)),
    ((None, 500), (2, KEY_VALUE), (3, KEY_VALUE), (4, KEY_VALUE), (5, KEY_VALUE), (2, QUERY), (3, QUERY), (4, QUERY), (5, QUERY)),
    ((None, 500), (3, KEY_VALUE), (2, KEY_VALUE), (5, KEY_VALUE), (4, KEY_VALUE), (3, QUERY), (2, QUERY), (5, QUERY), (4, QUERY)),
)
LATE_ORDER = (
    (),
    (),
    (),
    (),
    (),
    (),
    (),
    (),
    (),
    (),
    (),
    (),
    (),
    (),
    (),
    (),
)
SERVE_ORDER = (((1, 1), (3, 1), (2, 1), (0, 1)), ((2, 1), (0, 1), (3, 1), (1, 1)))
FINISH_ORDER = ((2, 3, 4, 5), (2, 3, 4, 5), (2, 3, 4, 5), (2, 3, 4, 5))


def notice(mine, theirs):
    if theirs // 2 > mine // 2:
        return theirs if mine % 2 == 0 else theirs | 1
    if mine % 2 == 0 and theirs % 2 and mine > 0:
        return mine + 1
    return None


def notices(mine):
    return {notice(mine, theirs) for theirs in WORKERS if theirs != mine} - {None}


def kernel(
    sections,
    stream_hbm, query_hbm, key_hbm, value_hbm, incoming_hbm,
    both_ref,
    stream_own, held, gathered, result, attended, stream_before, attended_before,
    load_sem, send_sem, recv_sem, query_sem, back_sem, before_sem, known_sem,
):
    updated_ref, received_ref = both_ref.at[0], both_ref.at[1]
    key_all, value_all, query_all = (gathered.at[kind] for kind in range(3))
    section = lax.axis_index("section")
    seq = lax.axis_index("seq")
    me = lax.rem(seq, GROUP)
    base = seq - me
    row, side = lax.div(me, 2), lax.rem(me, 2)
    width = gathered.shape[3]
    others = pl.ds(1, GROUP - 1)
    working = (me >= WORKERS[0]) & (me <= WORKERS[-1])
    last = section == sections - 1
    direct = (lax.rem(section, 2) == 0) & jnp.logical_not(last)
    behind = lax.rem(section, 2) == 1

    loads = [
        pltpu.make_async_copy(source, held.at[kind], load_sem.at[0])
        for kind, source in enumerate((key_hbm, value_hbm, query_hbm))
    ]
    for load in loads:
        load.start()

    def here(run):
        for mine in range(GROUP):

            @pl.when(me == mine)
            def _():
                run(mine)

    def signal(sem, place):
        pl.semaphore_signal(sem, inc=1, device_id={"seq": base + place}, device_id_type=MESH)

    barrier = pltpu.get_barrier_semaphore()

    def greet(mine):
        for theirs in range(GROUP):
            later = theirs // 2 > mine // 2 and (mine % 2 == 0 or theirs % 2)
            if later or theirs == mine + 1 - mine % 2 * 2 and (mine % 2 == 0 or mine == 1):
                signal(barrier, theirs)

    here(greet)

    @pl.when(section < sections - 1)
    def _():
        pl.semaphore_signal(barrier, inc=1, device_id={"section": section + 1}, device_id_type=MESH)

    stream_load = pltpu.make_async_copy(stream_hbm, stream_own, load_sem.at[1])
    stream_load.start()

    @pl.when(section == 0)
    def _():
        pltpu.make_async_copy(incoming_hbm, received_ref, recv_sem.at[1]).start()

    def exchange(kind, mine, theirs):
        return pltpu.make_async_remote_copy(
            src_ref=held.at[kind, :, pl.ds((theirs - WORKERS[0]) * width, width)],
            dst_ref=gathered.at[kind, mine ^ theirs],
            send_sem=send_sem.at[3 if kind == 2 else 0],
            recv_sem=query_sem.at[(mine ^ theirs) // 2] if kind == 2 else recv_sem.at[0],
            device_id={"seq": base + theirs},
            device_id_type=MESH,
        )

    def place_at(mask):
        place = 0
        for weight in (1, 2, 4):
            bit = lax.rem(lax.div(me, weight), 2)
            place = place + weight * ((1 - bit) if mask & weight else bit)
        return place

    def giving_back(mask):
        return pltpu.make_async_remote_copy(
            src_ref=result.at[mask],
            dst_ref=attended.at[me - WORKERS[0]],
            send_sem=send_sem.at[1],
            recv_sem=back_sem.at[me - WORKERS[0]],
            device_id={"seq": base + place_at(mask)},
            device_id_type=MESH,
        )

    def giving_ahead(mask):
        return pltpu.make_async_remote_copy(
            src_ref=result.at[mask],
            dst_ref=attended_before.at[me - WORKERS[0]],
            send_sem=send_sem.at[1 if mask else 4],
            recv_sem=before_sem.at[me - WORKERS[0]],
            device_id={"section": lax.rem(section + 1, sections), "seq": base + place_at(mask)},
            device_id_type=MESH,
        )

    def give(mask):
        if mask:

            @pl.when(jnp.logical_not(direct) | (me == mask))
            def _():
                giving_back(mask).start()

        @pl.when(direct)
        def _():
            giving_ahead(mask).start()

    def handing_on(worker):
        index = worker - WORKERS[0]
        return pltpu.make_async_remote_copy(
            src_ref=attended_before.at[index],
            dst_ref=attended.at[index],
            send_sem=send_sem.at[4],
            recv_sem=back_sem.at[index],
            device_id={"section": lax.rem(section + sections - 1, sections)},
            device_id_type=MESH,
        )

    def passing(cols):
        return pltpu.make_async_remote_copy(
            src_ref=updated_ref.at[:, cols],
            dst_ref=received_ref.at[:, cols],
            send_sem=send_sem.at[2],
            recv_sem=recv_sem.at[1],
            device_id={"section": lax.rem(section + 1, sections)},
            device_id_type=MESH,
        )

    def landed(ref, sem):
        pltpu.make_async_copy(ref, ref, sem).wait()

    greeted = jnp.where(side == 0, jnp.maximum(row, 1), 2 * row + 1)
    pl.semaphore_wait(barrier, greeted + jnp.where(section > 0, 1, 0))

    def answer(mine):
        for theirs in range(GROUP):
            if mine in notices(theirs):
                signal(known_sem.at[mine ^ theirs], theirs)

    here(answer)

    @pl.when(section > 0)
    def _():
        pl.semaphore_signal(
            known_sem.at[0], inc=1, device_id={"section": section - 1}, device_id_type=MESH
        )

    landed(held, load_sem.at[0])
    def send(orders, earlier):
        for number, order in enumerate(orders):
            mine, met = number % GROUP, {None}
            for theirs, _ in earlier[number]:
                if theirs is not None:
                    met.add(notice(mine, theirs))
            if order:

                @pl.when(me + GROUP * lax.rem(section, 2) == number)
                def _():
                    for theirs, kinds in order:
                        if theirs is None:
                            pl.delay(kinds)
                            continue
                        shown = notice(mine, theirs)
                        if shown not in met:
                            met.add(shown)
                            pl.semaphore_wait(known_sem.at[mine ^ shown], 1)
                        for kind in kinds:
                            exchange(kind, mine, theirs).start()

    @pl.when(direct)
    def _():
        pl.semaphore_wait(known_sem.at[0], 1)

    send(SEND_ORDER, [()] * len(SEND_ORDER))

    @pl.when(direct)
    def _():
        pltpu.make_async_remote_copy(
            src_ref=stream_hbm,
            dst_ref=stream_before,
            send_sem=send_sem.at[2],
            recv_sem=recv_sem.at[1],
            device_id={"section": lax.rem(section + 1, sections)},
            device_id_type=MESH,
        ).start()

    factor = HEAD_SIZE ** -0.5 * LOG2_E

    def attend(pair, count):
        at = pl.ds(2 * pair, 2 * count)
        for start in range(0, width, 2 * HEAD_SIZE):
            heads = [pl.ds(start + offset, HEAD_SIZE) for offset in (0, HEAD_SIZE)]
            scores = [
                lax.dot_general(
                    query_all[at, :, head].reshape(-1, HEAD_SIZE),
                    key_all[:, :, head].reshape(-1, HEAD_SIZE),
                    (((1,), (1,)), ((), ())),
                    preferred_element_type=jnp.float32,
                )
                for head in heads
            ]
            highest = [jnp.max(its, axis=-1, keepdims=True) for its in scores]
            exponent = [jnp.exp2((its - top) * factor) for its, top in zip(scores, highest)]
            totals = [jnp.sum(its, axis=-1, keepdims=True) for its in exponent]
            summed = [
                jnp.dot(
                    its.astype(jnp.bfloat16), value_all[:, :, head].reshape(-1, HEAD_SIZE),
                    preferred_element_type=jnp.float32,
                )
                for its, head in zip(exponent, heads)
            ]
            for its, total, head in zip(summed, totals, heads):
                out = (its * (1.0 / total)).astype(jnp.bfloat16)
                result[at, :, head] = out.reshape(2 * count, -1, HEAD_SIZE)

    @pl.when(working)
    def _():
        own = pl.ds(pl.multiple_of((me - WORKERS[0]) * width, HEAD_SIZE), width)
        for kind in range(3):
            gathered[kind, 0] = held[kind, :, own]
        landed(gathered.at[pl.ds(0, 2), others], recv_sem.at[0])

    @pl.when(jnp.logical_not(working))
    def _():
        landed(held.at[pl.ds(0, 2)], send_sem.at[0])

    send(LATE_ORDER, SEND_ORDER)

    for number, order in enumerate(SERVE_ORDER):

        @pl.when(row == WORKERS[0] // 2 + number)
        def _():
            for pair, count in order:
                for its in range(pair, pair + count):
                    landed(query_all.at[pl.ds(2 * its, 2) if its else pl.ds(1, 1)], query_sem.at[its])
                attend(pair, count)
                masks = range(2 * pair, 2 * (pair + count))
                for mask in masks:

                    @pl.when(me == mask)
                    def _():
                        give(mask)

                for mask in masks:

                    @pl.when(me != mask)
                    def _():
                        give(mask)

    landed(stream_own, load_sem.at[1])

    passes = jnp.logical_not(last | direct)

    @pl.when(passes)
    def _():
        pl.semaphore_wait(known_sem.at[0], 1)

    def plus(stream, piece):
        return (stream.astype(jnp.float32) + piece.astype(jnp.float32)).astype(jnp.bfloat16)

    def finish(worker):
        cols = pl.ds((worker - WORKERS[0]) * width, width)

        def update(piece):
            updated_ref[:, cols] = plus(stream_own[:, cols], piece)

        @pl.when(me == worker)
        def _():
            update(result[0])

        @pl.when(me != worker)
        def _():
            landed(attended.at[worker - WORKERS[0]], back_sem.at[worker - WORKERS[0]])
            update(attended[worker - WORKERS[0]])

        @pl.when(passes)
        def _():
            passing(cols).start()

    for order in sorted(set(FINISH_ORDER)):
        chosen = functools.reduce(
            jnp.logical_or, [row == number for number, its in enumerate(FINISH_ORDER) if its == order]
        )

        @pl.when(chosen)
        def _():
            for worker in order:
                finish(worker)

    @pl.when(behind)
    def _():
        landed(stream_before, recv_sem.at[1])
        for worker in (2, 3, 4, 5):
            index = worker - WORKERS[0]
            landed(attended_before.at[index], before_sem.at[index])

            @pl.when((me > 0) & (me != worker))
            def _():
                handing_on(worker).start()

            cols = pl.ds(index * width, width)
            received_ref[:, cols] = plus(stream_before[:, cols], attended_before[index])

        @pl.when(working)
        def _():
            landed(attended_before.at[pl.ds(1, len(WORKERS) - 1)], send_sem.at[4])

        @pl.when((me > 0) & jnp.logical_not(working))
        def _():
            landed(attended_before, send_sem.at[4])

    @pl.when(working)
    def _():
        most = pl.ds(0, (len(WORKERS) - 1) * width)
        landed(held.at[pl.ds(0, 2), :, most], send_sem.at[0])
        landed(held.at[2, :, most], send_sem.at[3])

        @pl.when(direct)
        def _():
            landed(result, send_sem.at[1])
            landed(result.at[0], send_sem.at[4])

        @pl.when(jnp.logical_not(direct))
        def _():
            landed(result.at[others], send_sem.at[1])

    @pl.when(jnp.logical_not(working))
    def _():
        landed(held.at[2], send_sem.at[3])

    @pl.when(section < sections - 1)
    def _():
        landed(updated_ref, send_sem.at[2])

    @pl.when(jnp.logical_not(behind))
    def _():
        landed(received_ref, recv_sem.at[1])


def per_device(sections, stream, queries, key_rows, values, incoming):
    rows, features = incoming.shape
    width = features // len(WORKERS)
    both = pl.pallas_call(
        functools.partial(kernel, sections),
        out_shape=pltpu.VMEM((2, rows, features), jnp.bfloat16),
        in_specs=[pl.BlockSpec(memory_space=pl.ANY)] * 5,
        out_specs=pl.BlockSpec(memory_space=pltpu.VMEM),
        scratch_shapes=[
            pltpu.VMEM((rows, features), jnp.bfloat16),
            pltpu.VMEM((3, rows, features), jnp.bfloat16),
            pltpu.VMEM((3, GROUP, rows, width), jnp.bfloat16),
            pltpu.VMEM((GROUP, rows, width), jnp.bfloat16),
            pltpu.VMEM((len(WORKERS), rows, width), jnp.bfloat16),
            pltpu.VMEM((rows, features), jnp.bfloat16),
            pltpu.VMEM((len(WORKERS), rows, width), jnp.bfloat16),
            pltpu.SemaphoreType.DMA((2,)),
            pltpu.SemaphoreType.DMA((5,)),
            pltpu.SemaphoreType.DMA((2,)),
            pltpu.SemaphoreType.DMA((GROUP // 2,)),
            pltpu.SemaphoreType.DMA((len(WORKERS),)),
            pltpu.SemaphoreType.DMA((len(WORKERS),)),
            pltpu.SemaphoreType.REGULAR((GROUP,)),
        ],
        compiler_params=pltpu.CompilerParams(collective_id=0, has_side_effects=True),
    )(stream[0], queries[0], key_rows[0], values[0], incoming)
    return both[:1], both[1:]


def solution(mesh):
    placed = (
        P("section", "seq", None),
        P("section", "seq", None),
        P("section", "seq", None),
        P("section", "seq", None),
        P("seq", None),
    )
    return jax.shard_map(
        functools.partial(per_device, mesh.shape["section"]),
        mesh=mesh,
        in_specs=placed,
        out_specs=(P("section", "seq", None), P("section", "seq", None)),
        check_vma=False,
    )
```
